32 devices in a mesh: py: 2 (over x), px: 4 (over z), pz: 4 (over y, core).
Axes of the slice: x: 2, y: 2, z: 4, core: 2. Of those that a mesh axis runs over, the one named last changes fastest.
Arguments:
- field_now: float32 [16, 64, 256, 128], P('py', 'px', 'pz'), may hold values from 0.2 to 1.8
- earlier: float32 [16, 64, 256, 128], P('py', 'px', 'pz'), may hold values from 0.2 to 1.8
- speed_square: float32 [16, 64, 256, 128], P('py', 'px', 'pz'), may hold values from 0.05 to 0.3
Outputs:
- column_sum: float32 [16, 64, 256, 128], P('py', 'px', 'pz')
- field_now_end: float32 [16, 64, 256, 128], P('py', 'px', 'pz')
The draws below stay inside these ranges and needn't reach their ends.
All inputs are finite; a program needn't handle non-finite values.
Results may differ from the reference program's by a relative error of at most 0.00002.
Values sent between devices are 32-bit elements; how exact they have to be, the bound alone decides.
A program may use at most 128 MiB of HBM per device.

```python
import jax
import jax.numpy as jnp
from jax import lax

GRID_J = 16
GRID_I = 64
GRID_K = 256
LEVELS = 128
STEPS = 4


def shard_levels(key, extent, split, low, top_value):
    level = 1.0
    for position, shards_of in split:
        heights = jax.random.uniform(jax.random.fold_in(jax.random.fold_in(key, 6), position), (shards_of,), jnp.float32, low / len(split), top_value / len(split))
        level = level * jnp.repeat(jnp.exp(heights), extent[position] // shards_of).reshape((-1,) + (1,) * (len(extent) - 1 - position))
    return level


def setup_inputs(seed: int = 0) -> dict:
    seeds = jax.random.split(jax.random.key(seed), 4)
    field_now = jnp.clip(0.2 + 1.5999999 * jax.random.uniform(seeds[0], (GRID_J, GRID_I, GRID_K, LEVELS), jnp.float32) ** shard_levels(seeds[0], (GRID_J, GRID_I, GRID_K, LEVELS), ((0, 2), (1, 4), (2, 4)), -0.2, 0.2), 0.2, 1.8)
    earlier = jnp.clip(0.2 + 1.5999999 * jax.random.uniform(seeds[1], (GRID_J, GRID_I, GRID_K, LEVELS), jnp.float32) ** shard_levels(seeds[1], (GRID_J, GRID_I, GRID_K, LEVELS), ((0, 2), (1, 4), (2, 4)), -0.2, 0.2), 0.2, 1.8)
    speed_square = jnp.clip(0.05 + 0.25 * jax.random.uniform(seeds[2], (GRID_J, GRID_I, GRID_K, LEVELS), jnp.float32) ** shard_levels(seeds[2], (GRID_J, GRID_I, GRID_K, LEVELS), ((0, 2), (1, 4), (2, 4)), -0.2, 0.2), 0.05, 0.3)
    return dict(field_now=field_now, earlier=earlier, speed_square=speed_square)


def without_rim(values, dims):
    for dim in dims:
        values = lax.slice_in_dim(values, 1, values.shape[dim] - 1, axis=dim)
    return values


def shifted_cells(values, dim, start, dims):
    others = [other for other in dims if other != dim]
    values = without_rim(values, others)
    return lax.slice_in_dim(values, start, start + values.shape[dim] - 2, axis=dim)


def march_step(padded, before, speed_square):
    middle = without_rim(padded, (0, 1, 2))
    lower = [shifted_cells(padded, dim, 0, (0, 1, 2)) for dim in (0, 1, 2)]
    upper = [shifted_cells(padded, dim, 2, (0, 1, 2)) for dim in (0, 1, 2)]
    spread = lower[0] + upper[0] + lower[1] + upper[1] + lower[2] + upper[2] - 6.0 * middle
    return 2.0 * middle - before + speed_square * spread


def reference(field_now, earlier, speed_square):
    for step in range(STEPS):
        later = march_step(jnp.pad(field_now, ((1, 1), (1, 1), (1, 1), (0, 0)), mode="wrap"), earlier, speed_square)
        earlier, field_now = field_now, later
    column_sum = jnp.cumsum(field_now, axis=0) / GRID_J
    return column_sum, field_now
```

```python
import functools

import jax
import jax.numpy as jnp
from jax import lax
from jax.experimental import pallas as pl
from jax.experimental.pallas import tpu as pltpu
from jax.sharding import PartitionSpec as P

STEPS = 4
CHUNKS = 2
OUT_CHUNKS = 4
MESH = pl.DeviceIdType.MESH


def march_kernel(
    peers, chunks, field, before, speed, end, under,
    u, cs, total, below, ysend, yrecv,
    load_sem, x_send, x_recv, z_send, z_recv, y_send, y_recv, t_send, t_recv, word, ready,
):
    J, I, K, L = field.shape
    ny, nx, nz = peers
    width = I // chunks
    my, mx, mz = (lax.axis_index(a) for a in ("py", "px", "pz"))
    y_side = ({"py": lax.rem(my + 1, ny)}, {"py": lax.rem(my + ny - 1, ny)})
    x_side = ({"px": lax.rem(mx + 1, nx)}, {"px": lax.rem(mx + nx - 1, nx)})
    z_side = ({"pz": lax.rem(mz + 1, nz)}, {"pz": lax.rem(mz + nz - 1, nz)})
    parts = ((1, J - 2), (0, 1), (J - 1, 1))

    loads = [
        pltpu.make_async_copy(
            field.at[pl.ds(start, size)], u.at[0, pl.ds(start + 1, size), pl.ds(1, I)], load_sem.at[part]
        )
        for part, (start, size) in reversed(tuple(enumerate(parts)))
    ] + [
        pltpu.make_async_copy(before, u.at[1, pl.ds(1, J), pl.ds(1, I)], load_sem.at[3]),
        pltpu.make_async_copy(speed, cs, load_sem.at[4]),
    ]
    barrier = pltpu.get_barrier_semaphore()
    above, under_me = mx < nx - 1, mx > 0
    pairs = [(mx < nx - 1, x_side[0], mx > 0, x_side[1])]
    if nz > 1:
        pairs.append((mz < nz - 1, z_side[0], mz > 0, z_side[1]))
    if nz > 2:
        pairs.append((mz == 0, z_side[1], mz == nz - 1, z_side[0]))

    def greet(to):
        pl.semaphore_signal(barrier, inc=1, device_id=to, device_id_type=MESH)

    for d in range(1, ny):
        greet({"py": lax.rem(my + d, ny)})
    expected = ny - 1
    for has_upper, upper, has_lower, _ in pairs:
        @pl.when(has_upper)
        def _(upper=upper):
            greet(upper)

        expected = expected + jnp.where(has_lower, 1, 0)

    for load in loads[:2]:
        load.start()
    pl.semaphore_wait(barrier, expected)

    def meet():
        for n, (_, _, has_lower, lower) in enumerate(pairs):
            @pl.when(has_lower)
            def _(n=n, lower=lower):
                pl.semaphore_signal(ready.at[n], inc=1, device_id=lower, device_id_type=MESH)

        for n, (has_upper, _, _, _) in enumerate(pairs):
            @pl.when(has_upper)
            def _(n=n):
                pl.semaphore_wait(ready.at[n], 1)

    def hand_on():
        for way, (comes, goes) in enumerate(((under_me, above), (above, under_me))):
            @pl.when(comes)
            def _(way=way):
                pl.semaphore_wait(word.at[way], 1)

            @pl.when(goes)
            def _(way=way):
                pl.semaphore_signal(word.at[way], inc=1, device_id=x_side[way], device_id_type=MESH)

    def remote(src, dst, send, recv, to):
        return pltpu.make_async_remote_copy(
            src_ref=src, dst_ref=dst, send_sem=send, recv_sem=recv, device_id=to, device_id_type=MESH
        )

    def order(t):
        return (0, 1) if t % 2 == 0 else (1, 0)

    def cuts(t, side):
        n = chunks if t + 1 == STEPS and side == order(t)[1] else 1
        return range(n), I // n

    def j_copy(t, side, c):
        row, rim = ((J - 1, 0), (0, J + 1))[side]
        size = cuts(t, side)[1]
        there = pl.ds(1 + c * size, size)
        return remote(u.at[t % 2, row + 1, there], u.at[t % 2, rim, there], x_send.at[t, side, c], x_recv.at[t, side, c], y_side[side])

    def i_copy(t, side, part):
        plane, rim = ((I - 1, 0), (0, I + 1))[side]
        start, size = parts[part]
        rows = pl.ds(start + 1, size)
        src = field.at[pl.ds(start, size), plane] if t == 0 else u.at[t % 2, rows, plane + 1]
        return remote(src, u.at[t % 2, rows, rim], z_send.at[t, side, part], z_recv.at[t, side, part], x_side[side])

    def k_copy(t, side, part):
        start, size = parts[part]
        rows = pl.ds(start, size)
        return remote(
            ysend.at[t, side, rows], yrecv.at[t, side, rows],
            y_send.at[t, side, part], y_recv.at[t, side, part], z_side[side],
        )

    def pack(t, j, i, value):
        ysend[t, 0, j, pl.ds(i, 1), :] = value[K - 1:K]
        ysend[t, 1, j, pl.ds(i, 1), :] = value[0:1]

    loads[0].wait()
    j_copy(0, 0, 0).start()
    loads[1].wait()
    j_copy(0, 1, 0).start()
    for load in loads[2:]:
        load.start()
    meet()
    hand_on()
    for part in range(3):
        for side in (0, 1):
            i_copy(0, side, part).start()

    loads[2].wait()

    def pack_row(j, carry):
        for i in range(I):
            ysend[0, 0, j, i:i + 1, :] = u[0, j + 1, i + 1, K - 1:K, :]
            ysend[0, 1, j, i:i + 1, :] = u[0, j + 1, i + 1, 0:1, :]
        return carry

    lax.fori_loop(0, J, pack_row, 0)
    for part in range(3):
        for side in (0, 1):
            k_copy(0, side, part).start()
    loads[3].wait()
    loads[4].wait()

    k_index = lax.broadcasted_iota(jnp.int32, (K, L), 0)

    def column(t, j, i):
        now, other = t % 2, (t + 1) % 2
        middle = u[now, j + 1, i + 1]
        low = jnp.where(k_index == 0, yrecv[t, 0, j, pl.ds(i, 1), :], pltpu.roll(middle, 1, 0))
        high = jnp.where(k_index == K - 1, yrecv[t, 1, j, pl.ds(i, 1), :], pltpu.roll(middle, K - 1, 0))
        spread = (
            u[now, j, i + 1] + u[now, j + 2, i + 1] + u[now, j + 1, i] + u[now, j + 1, i + 2]
            + low + high - 6.0 * middle
        )
        later = 2.0 * middle - u[other, j + 1, i + 1] + cs[j, i] * spread
        if t + 1 < STEPS:
            u[other, j + 1, i + 1] = later
            pack(t + 1, j, i, later)
        else:
            end[j, i] = later

    def total_copy(d, c):
        here = pl.ds(c * width, width)
        return remote(
            total.at[here], below.at[d - 1, here], t_send.at[d - 1, c], t_recv.at[d - 1, c],
            {"py": lax.rem(my + d, ny)},
        )

    for t in range(STEPS):
        last = t + 1 == STEPS
        for side in (0, 1):
            i_copy(t, side, 0).wait_recv()
            k_copy(t, side, 0).wait_recv()
            if t > 0:
                i_copy(t - 1, side, 0).wait_send()

        def inner(q, carry, t=t):
            j = 1 + q // (I // 2)
            i = lax.rem(q, I // 2) * 2
            column(t, j, i)
            column(t, j, i + 1)
            return carry

        lax.fori_loop(0, (J - 2) * (I // 2), inner, 0)
        if not last:
            for side in (0, 1):
                i_copy(t + 1, side, 0).start()
                k_copy(t + 1, side, 0).start()

        for s in order(t):
            row, part = ((0, 1), (J - 1, 2))[s]
            for side in (0, 1):
                i_copy(t, side, part).wait_recv()
                k_copy(t, side, part).wait_recv()
                if t > 0:
                    i_copy(t - 1, side, part).wait_send()
            if t > 0:
                j_copy(t - 1, 1 - s, 0).wait_send()

            def outer(i, carry, t=t, row=row):
                column(t, row, i)
                return carry

            if not last:
                j_copy(t, s, 0).wait_recv()
                pieces, size = cuts(t + 1, 1 - s)
                for c in pieces:
                    lax.fori_loop(c * size, (c + 1) * size, outer, 0)
                    j_copy(t + 1, 1 - s, c).start()
                for side in (0, 1):
                    i_copy(t + 1, side, part).start()
                    k_copy(t + 1, side, part).start()
            else:
                pieces, size = cuts(t, s)
                for c in pieces:
                    j_copy(t, s, c).wait_recv()
                    lax.fori_loop(c * size, (c + 1) * size, outer, 0)
                    if s == order(t)[1]:
                        def add_up(i, carry):
                            value = end[0, i]
                            for j in range(1, J):
                                value = value + end[j, i]
                            total[i] = value
                            return carry

                        lax.fori_loop(c * size, (c + 1) * size, add_up, 0)
                        for d in range(1, ny):
                            @pl.when(my + d < ny)
                            def _(d=d, c=c):
                                total_copy(d, c).start()

    for c in range(chunks):
        here = pl.ds(c * width, width)
        under[here] = jnp.zeros((width, K, L), jnp.float32)
        for d in range(1, ny):
            @pl.when(my >= d)
            def _(d=d, c=c, here=here):
                total_copy(d, c).wait_recv()
                under[here] = under[here] + below[d - 1, here]

    for side in (0, 1):
        for c in cuts(STEPS - 1, side)[0]:
            j_copy(STEPS - 1, side, c).wait_send()
        for part in range(3):
            i_copy(STEPS - 1, side, part).wait_send()
            for t in range(STEPS):
                k_copy(t, side, part).wait_send()
    for c in range(chunks):
        for d in range(1, ny):
            @pl.when(my + d < ny)
            def _(d=d, c=c):
                total_copy(d, c).wait_send()


def sums_kernel(scale, chunks, end, under, sums_out, field_out, csum, sum_sem, out_sem):
    J, I = end.shape[:2]
    width = I // chunks

    def out_copy(c):
        here = pl.ds(c * width, width)
        return pltpu.make_async_copy(end.at[:, here], field_out.at[:, here], out_sem.at[c])

    def sum_copy(c):
        here = pl.ds(c * width, width)
        return pltpu.make_async_copy(csum.at[:, here], sums_out.at[:, here], sum_sem.at[c])

    for c in range(chunks):
        out_copy(c).start()
    for c in range(chunks):
        def running(q, carry, c=c):
            i = c * width + q
            value = under[i]
            for j in range(J):
                value = value + end[j, i]
                csum[j, i] = value * scale
            return carry

        lax.fori_loop(0, width, running, 0)
        sum_copy(c).start()
    for c in range(chunks):
        out_copy(c).wait()
        sum_copy(c).wait()


def local(peers, field_now, earlier, speed_square):
    J, I, K, L = field_now.shape
    chunks = CHUNKS if I % CHUNKS == 0 else 1
    out_chunks = OUT_CHUNKS if I % OUT_CHUNKS == 0 else 1
    ny = peers[0]
    f32 = jnp.float32
    dma = pltpu.SemaphoreType.DMA
    anywhere = pl.BlockSpec(memory_space=pltpu.MemorySpace.HBM)
    shape = jax.ShapeDtypeStruct(field_now.shape, f32)
    slots = max(ny - 1, 1)
    resident = pl.BlockSpec(memory_space=pltpu.VMEM)
    end, under = pl.pallas_call(
        functools.partial(march_kernel, peers, chunks),
        out_shape=(pltpu.VMEM((J, I, K, L), f32), pltpu.VMEM((I, K, L), f32)),
        in_specs=[anywhere] * 3,
        out_specs=(resident, resident),
        scratch_shapes=[
            pltpu.VMEM((2, J + 2, I + 2, K, L), f32),
            pltpu.VMEM((J, I, K, L), f32),
            pltpu.VMEM((I, K, L), f32),
            pltpu.VMEM((slots, I, K, L), f32),
            pltpu.VMEM((STEPS, 2, J, I, L), f32),
            pltpu.VMEM((STEPS, 2, J, I, L), f32),
            dma((5,)),
            dma((STEPS, 2, chunks)),
            dma((STEPS, 2, chunks)),
            dma((STEPS, 2, 3)),
            dma((STEPS, 2, 3)),
            dma((STEPS, 2, 3)),
            dma((STEPS, 2, 3)),
            dma((slots, chunks)),
            dma((slots, chunks)),
            pltpu.SemaphoreType.REGULAR((2,)),
            pltpu.SemaphoreType.REGULAR((3,)),
        ],
        compiler_params=pltpu.CompilerParams(
            collective_id=0, has_side_effects=True, vmem_limit_bytes=55 * 1024 * 1024
        ),
        name="march",
    )(field_now, earlier, speed_square)
    return pl.pallas_call(
        functools.partial(sums_kernel, 1.0 / (J * ny), out_chunks),
        out_shape=(shape, shape),
        in_specs=[resident] * 2,
        out_specs=(anywhere, anywhere),
        scratch_shapes=[pltpu.VMEM((J, I, K, L), f32), dma((out_chunks,)), dma((out_chunks,))],
        compiler_params=pltpu.CompilerParams(vmem_limit_bytes=16 * 1024 * 1024),
        name="sums",
    )(end, under)


def solution(mesh):
    placed = P("py", "px", "pz", None)
    peers = tuple(mesh.shape[a] for a in ("py", "px", "pz"))
    return jax.shard_map(
        functools.partial(local, peers),
        mesh=mesh,
        in_specs=(placed,) * 3,
        out_specs=(placed,) * 2,
        check_vma=False,
    )
```

```python
import functools

import jax
import jax.numpy as jnp
from jax import lax
from jax.experimental import pallas as pl
from jax.experimental.pallas import tpu as pltpu
from jax.sharding import PartitionSpec as P

STEPS = 4
OUT_CHUNKS = 4
FIRST = (1, 2)
MESH = pl.DeviceIdType.MESH


def march_kernel(
    peers, split, field, before, speed, end, under, total,
    u, cs, below, ysend, yrecv,
    load_sem, x_send, x_recv, z_send, z_recv, y_send, y_recv, t_send, t_recv, word, ready,
):
    J, I, K, L = field.shape
    ny, nx, nz = peers
    my, mx, mz = (lax.axis_index(a) for a in ("py", "px", "pz"))
    y_side = ({"py": lax.rem(my + 1, ny)}, {"py": lax.rem(my + ny - 1, ny)})
    x_side = ({"px": lax.rem(mx + 1, nx)}, {"px": lax.rem(mx + nx - 1, nx)})
    z_side = ({"pz": lax.rem(mz + 1, nz)}, {"pz": lax.rem(mz + nz - 1, nz)})
    parts = ((1, J - 2), (0, 1), (J - 1, 1))
    halves = ((0, split), (split, I - split))
    second_core = lax.rem(mz, 2) == 1

    loads = [
        pltpu.make_async_copy(
            field.at[pl.ds(start, size)], u.at[0, pl.ds(start + 1, size), pl.ds(1, I)], load_sem.at[part]
        )
        for part, (start, size) in reversed(tuple(enumerate(parts)))
    ] + [
        pltpu.make_async_copy(before, u.at[1, pl.ds(1, J), pl.ds(1, I)], load_sem.at[3]),
        pltpu.make_async_copy(speed, cs, load_sem.at[4]),
    ]
    barrier = pltpu.get_barrier_semaphore()
    above, under_me = mx < nx - 1, mx > 0
    pairs = [(mx < nx - 1, x_side[0], mx > 0, x_side[1])]
    if nz > 1:
        pairs.append((mz < nz - 1, z_side[0], mz > 0, z_side[1]))
    if nz > 2:
        pairs.append((mz == 0, z_side[1], mz == nz - 1, z_side[0]))

    def greet(to):
        pl.semaphore_signal(barrier, inc=1, device_id=to, device_id_type=MESH)

    for d in range(1, ny):
        greet({"py": lax.rem(my + d, ny)})
    expected = ny - 1
    for has_upper, upper, has_lower, _ in pairs:
        @pl.when(has_upper)
        def _(upper=upper):
            greet(upper)

        expected = expected + jnp.where(has_lower, 1, 0)

    for load in loads[:2]:
        load.start()
    pl.semaphore_wait(barrier, expected)

    def meet():
        for n, (_, _, has_lower, lower) in enumerate(pairs):
            @pl.when(has_lower)
            def _(n=n, lower=lower):
                pl.semaphore_signal(ready.at[n], inc=1, device_id=lower, device_id_type=MESH)

        for n, (has_upper, _, _, _) in enumerate(pairs):
            @pl.when(has_upper)
            def _(n=n):
                pl.semaphore_wait(ready.at[n], 1)

    def hand_on():
        for way, (comes, goes) in enumerate(((under_me, above), (above, under_me))):
            @pl.when(comes)
            def _(way=way):
                pl.semaphore_wait(word.at[way], 1)

            @pl.when(goes)
            def _(way=way):
                pl.semaphore_signal(word.at[way], inc=1, device_id=x_side[way], device_id_type=MESH)

    def remote(src, dst, send, recv, to):
        return pltpu.make_async_remote_copy(
            src_ref=src, dst_ref=dst, send_sem=send, recv_sem=recv, device_id=to, device_id_type=MESH
        )

    def order(t):
        return (0, 1) if t % 2 == 0 else (1, 0)

    def cuts(t, side):
        return halves if t + 1 == STEPS and side == order(t)[1] else ((0, I),)

    def j_copy(t, side, c):
        row, rim = ((J - 1, 0), (0, J + 1))[side]
        start, size = cuts(t, side)[c]
        there = pl.ds(1 + start, size)
        return remote(u.at[t % 2, row + 1, there], u.at[t % 2, rim, there], x_send.at[t, side, c], x_recv.at[t, side, c], y_side[side])

    def i_copy(t, side, part):
        plane, rim = ((I - 1, 0), (0, I + 1))[side]
        start, size = parts[part]
        rows = pl.ds(start + 1, size)
        src = field.at[pl.ds(start, size), plane] if t == 0 else u.at[t % 2, rows, plane + 1]
        return remote(src, u.at[t % 2, rows, rim], z_send.at[t, side, part], z_recv.at[t, side, part], x_side[side])

    def k_copy(t, side, part):
        start, size = parts[part]
        rows = pl.ds(start, size)
        return remote(
            ysend.at[t, side, rows], yrecv.at[t, side, rows],
            y_send.at[t, side, part], y_recv.at[t, side, part], z_side[side],
        )

    def pack(t, j, i, value):
        ysend[t, 0, j, pl.ds(i, 1), :] = value[K - 1:K]
        ysend[t, 1, j, pl.ds(i, 1), :] = value[0:1]

    loads[0].wait()
    j_copy(0, 0, 0).start()
    loads[1].wait()
    j_copy(0, 1, 0).start()
    for load in loads[2:]:
        load.start()
    meet()
    hand_on()
    for part in range(3):
        for side in (0, 1):
            i_copy(0, side, part).start()

    loads[2].wait()

    def pack_row(j, carry):
        for i in range(I):
            ysend[0, 0, j, i:i + 1, :] = u[0, j + 1, i + 1, K - 1:K, :]
            ysend[0, 1, j, i:i + 1, :] = u[0, j + 1, i + 1, 0:1, :]
        return carry

    lax.fori_loop(0, J, pack_row, 0)
    for part in range(3):
        for side in (0, 1):
            k_copy(0, side, part).start()
    loads[3].wait()
    loads[4].wait()

    k_index = lax.broadcasted_iota(jnp.int32, (K, L), 0)

    def column(t, j, i):
        now, other = t % 2, (t + 1) % 2
        middle = u[now, j + 1, i + 1]
        low = jnp.where(k_index == 0, yrecv[t, 0, j, pl.ds(i, 1), :], pltpu.roll(middle, 1, 0))
        high = jnp.where(k_index == K - 1, yrecv[t, 1, j, pl.ds(i, 1), :], pltpu.roll(middle, K - 1, 0))
        spread = (
            u[now, j, i + 1] + u[now, j + 2, i + 1] + u[now, j + 1, i] + u[now, j + 1, i + 2]
            + low + high - 6.0 * middle
        )
        later = 2.0 * middle - u[other, j + 1, i + 1] + cs[j, i] * spread
        if t + 1 < STEPS:
            u[other, j + 1, i + 1] = later
            pack(t + 1, j, i, later)
        else:
            end[j, i] = later

    def total_copy(d, first):
        here = pl.ds(0, split if first else I)
        return remote(
            total.at[here], below.at[d - 1, here], t_send.at[d - 1], t_recv.at[d - 1], {"py": lax.rem(my + d, ny)}
        )

    def for_totals(mine, first, act):
        for d in range(1, ny):
            @pl.when(jnp.logical_and(second_core if first else jnp.logical_not(second_core), my + d < ny if mine else my >= d))
            def _(d=d):
                act(total_copy(d, first), d)

    for t in range(STEPS):
        last = t + 1 == STEPS
        for side in (0, 1):
            i_copy(t, side, 0).wait_recv()
            k_copy(t, side, 0).wait_recv()
            if t > 0:
                i_copy(t - 1, side, 0).wait_send()

        def inner(q, carry, t=t):
            j = 1 + q // (I // 2)
            i = lax.rem(q, I // 2) * 2
            column(t, j, i)
            column(t, j, i + 1)
            return carry

        lax.fori_loop(0, (J - 2) * (I // 2), inner, 0)
        if not last:
            for side in (0, 1):
                i_copy(t + 1, side, 0).start()
                k_copy(t + 1, side, 0).start()

        for s in order(t):
            row, part = ((0, 1), (J - 1, 2))[s]
            for side in (0, 1):
                i_copy(t, side, part).wait_recv()
                k_copy(t, side, part).wait_recv()
                if t > 0:
                    i_copy(t - 1, side, part).wait_send()
            if t > 0:
                j_copy(t - 1, 1 - s, 0).wait_send()

            def outer(i, carry, t=t, row=row, s=s):
                column(t, row, i)
                if t + 1 == STEPS and s == order(t)[1]:
                    total[i] = total[i] + end[row, i]
                return carry

            if last and s == order(t)[1]:
                def add_up(i, carry, row=row):
                    value, *others = (end[j, i] for j in range(J) if j != row)
                    for other in others:
                        value = value + other
                    total[i] = value
                    return carry

                lax.fori_loop(0, I, add_up, 0)

            if not last:
                j_copy(t, s, 0).wait_recv()
                for c, (start, size) in enumerate(cuts(t + 1, 1 - s)):
                    lax.fori_loop(start, start + size, outer, 0)
                    j_copy(t + 1, 1 - s, c).start()
                for side in (0, 1):
                    i_copy(t + 1, side, part).start()
                    k_copy(t + 1, side, part).start()
            else:
                for c, (start, size) in enumerate(cuts(t, s)):
                    j_copy(t, s, c).wait_recv()
                    lax.fori_loop(start, start + size, outer, 0)
                    if s == order(t)[1]:
                        for_totals(True, c == 0, lambda copy, d: copy.start())

    under[...] = jnp.zeros((I, K, L), jnp.float32)
    for first in (True, False):
        def take(copy, d, size=split if first else I):
            copy.wait_recv()
            under[:size] = under[:size] + below[d - 1, :size]

        for_totals(False, first, take)

    for side in (0, 1):
        for c in range(len(cuts(STEPS - 1, side))):
            j_copy(STEPS - 1, side, c).wait_send()
        for part in range(3):
            i_copy(STEPS - 1, side, part).wait_send()
            for t in range(STEPS):
                k_copy(t, side, part).wait_send()
    for first in (True, False):
        for_totals(True, first, lambda copy, d: copy.wait_send())


def rest_kernel(ny, split, total, under, _, under_rest, below, send, recv):
    size = total.shape[0] - split
    my = lax.axis_index("py")
    there = pl.ds(split, size)
    second_core = lax.rem(lax.axis_index("pz"), 2) == 1

    def copy(d):
        return pltpu.make_async_remote_copy(
            src_ref=total.at[there], dst_ref=below.at[d - 1], send_sem=send.at[d - 1], recv_sem=recv.at[d - 1],
            device_id={"py": lax.rem(my + d, ny)}, device_id_type=MESH,
        )

    under_rest[...] = under[split:]

    @pl.when(second_core)
    def _():
        barrier = pltpu.get_barrier_semaphore()
        for d in range(1, ny):
            @pl.when(my >= d)
            def _(d=d):
                pl.semaphore_signal(barrier, inc=1, device_id={"py": lax.rem(my + ny - d, ny)}, device_id_type=MESH)

        @pl.when(my < ny - 1)
        def _():
            pl.semaphore_wait(barrier, ny - 1 - my)

        for d in range(1, ny):
            @pl.when(my + d < ny)
            def _(d=d):
                copy(d).start()

        for d in range(1, ny):
            @pl.when(my >= d)
            def _(d=d):
                copy(d).wait_recv()
                under_rest[...] = under_rest[...] + below[d - 1]

        for d in range(1, ny):
            @pl.when(my + d < ny)
            def _(d=d):
                copy(d).wait_send()


def columns_out(scale, chunks, start, size, end, under, sums_out, csum, sem):
    J = end.shape[0]
    width = size // chunks

    def sum_copy(c):
        here = pl.ds(c * width, width)
        return pltpu.make_async_copy(csum.at[:, here], sums_out.at[:, pl.ds(start + c * width, width)], sem.at[c])

    for c in range(chunks):
        def running(i, carry):
            value = under[i]
            for j in range(J):
                value = value + end[j, start + i]
                csum[j, i] = value * scale
            return carry

        lax.fori_loop(c * width, (c + 1) * width, running, 0)
        sum_copy(c).start()
    return [sum_copy(c) for c in range(chunks)]


def first_out_kernel(scale, chunks, split, end, under, sums_out, field_out, done, csum, sem, field_sem):
    whole = pltpu.make_async_copy(end, field_out, field_sem)
    whole.start()
    second_core = lax.rem(lax.axis_index("pz"), 2) == 1

    def columns(size):
        for copy in columns_out(scale, chunks, 0, size, end, under, sums_out, csum, sem):
            copy.wait()

    @pl.when(second_core)
    def _():
        columns(split)

    @pl.when(jnp.logical_not(second_core))
    def _():
        columns(end.shape[1])

    whole.wait()
    done[...] = jnp.zeros(done.shape, jnp.float32)


def rest_out_kernel(scale, chunks, split, end, under_rest, _, sums_out, csum, sem):
    @pl.when(lax.rem(lax.axis_index("pz"), 2) == 1)
    def _():
        for copy in columns_out(scale, chunks, split, end.shape[1] - split, end, under_rest, sums_out, csum, sem):
            copy.wait()


def local(peers, field_now, earlier, speed_square):
    J, I, K, L = field_now.shape
    ny = peers[0]
    split = I * FIRST[0] // FIRST[1]
    f32 = jnp.float32
    dma = pltpu.SemaphoreType.DMA
    anywhere = pl.BlockSpec(memory_space=pltpu.MemorySpace.HBM)
    shape = jax.ShapeDtypeStruct(field_now.shape, f32)
    slots = max(ny - 1, 1)
    resident = pl.BlockSpec(memory_space=pltpu.VMEM)
    end, under, total = pl.pallas_call(
        functools.partial(march_kernel, peers, split),
        out_shape=(pltpu.VMEM((J, I, K, L), f32), pltpu.VMEM((I, K, L), f32), pltpu.VMEM((I, K, L), f32)),
        in_specs=[anywhere] * 3,
        out_specs=(resident,) * 3,
        scratch_shapes=[
            pltpu.VMEM((2, J + 2, I + 2, K, L), f32),
            pltpu.VMEM((J, I, K, L), f32),
            pltpu.VMEM((slots, I, K, L), f32),
            pltpu.VMEM((STEPS, 2, J, I, L), f32),
            pltpu.VMEM((STEPS, 2, J, I, L), f32),
            dma((5,)),
            dma((STEPS, 2, 2)),
            dma((STEPS, 2, 2)),
            dma((STEPS, 2, 3)),
            dma((STEPS, 2, 3)),
            dma((STEPS, 2, 3)),
            dma((STEPS, 2, 3)),
            dma((slots,)),
            dma((slots,)),
            pltpu.SemaphoreType.REGULAR((2,)),
            pltpu.SemaphoreType.REGULAR((3,)),
        ],
        compiler_params=pltpu.CompilerParams(
            collective_id=0, has_side_effects=True, vmem_limit_bytes=56 * 1024 * 1024
        ),
        name="march",
    )(field_now, earlier, speed_square)
    scale = 1.0 / (J * ny)
    small = pltpu.CompilerParams(vmem_limit_bytes=16 * 1024 * 1024)

    chunks = OUT_CHUNKS if I % OUT_CHUNKS == 0 and split % OUT_CHUNKS == 0 else 1

    sums, field_end, done = pl.pallas_call(
        functools.partial(first_out_kernel, scale, chunks, split),
        out_shape=(shape, shape, pltpu.VMEM((8, L), f32)),
        in_specs=[resident] * 2,
        out_specs=(anywhere, anywhere, resident),
        scratch_shapes=[pltpu.VMEM((J, I, K, L), f32), dma((chunks,)), dma],
        compiler_params=small,
        name="first_out",
    )(end, under)
    rest = I - split
    under_rest = pl.pallas_call(
        functools.partial(rest_kernel, ny, split),
        out_shape=pltpu.VMEM((rest, K, L), f32),
        in_specs=[resident] * 3,
        out_specs=resident,
        scratch_shapes=[pltpu.VMEM((slots, rest, K, L), f32), dma((slots,)), dma((slots,))],
        compiler_params=pltpu.CompilerParams(
            collective_id=1, has_side_effects=True, vmem_limit_bytes=16 * 1024 * 1024
        ),
        name="rest",
    )(total, under, done)
    sums = pl.pallas_call(
        functools.partial(rest_out_kernel, scale, chunks, split),
        out_shape=shape,
        in_specs=[resident] * 2 + [anywhere],
        out_specs=anywhere,
        input_output_aliases={2: 0},
        scratch_shapes=[pltpu.VMEM((J, rest, K, L), f32), dma((chunks,))],
        compiler_params=small,
        name="rest_out",
    )(end, under_rest, sums)
    return sums, field_end


def solution(mesh):
    placed = P("py", "px", "pz", None)
    peers = tuple(mesh.shape[a] for a in ("py", "px", "pz"))
    return jax.shard_map(
        functools.partial(local, peers),
        mesh=mesh,
        in_specs=(placed,) * 3,
        out_specs=(placed,) * 2,
        check_vma=False,
    )
```

```python
import functools

import jax
import jax.numpy as jnp
from jax import lax
from jax.experimental import pallas as pl
from jax.experimental.pallas import tpu as pltpu
from jax.sharding import PartitionSpec as P

STEPS = 4
OUT_CHUNKS = 4
FIRST = (1, 2)
MESH = pl.DeviceIdType.MESH


def march_kernel(
    peers, split, field, before, speed, end, under, total,
    u, cs, below, ysend, yrecv,
    load_sem, x_send, x_recv, z_send, z_recv, y_send, y_recv, t_send, t_recv, word, ready,
):
    J, I, K, L = field.shape
    ny, nx, nz = peers
    my, mx, mz = (lax.axis_index(a) for a in ("py", "px", "pz"))
    y_side = ({"py": lax.rem(my + 1, ny)}, {"py": lax.rem(my + ny - 1, ny)})
    x_side = ({"px": lax.rem(mx + 1, nx)}, {"px": lax.rem(mx + nx - 1, nx)})
    z_side = ({"pz": lax.rem(mz + 1, nz)}, {"pz": lax.rem(mz + nz - 1, nz)})
    parts = ((1, J - 2), (0, 1), (J - 1, 1))
    halves = ((0, split), (split, I - split))
    second_core = lax.rem(mz, 2) == 1

    loads = [
        pltpu.make_async_copy(
            field.at[pl.ds(start, size)], u.at[0, pl.ds(start + 1, size), pl.ds(1, I)], load_sem.at[part]
        )
        for part, (start, size) in reversed(tuple(enumerate(parts)))
    ] + [
        pltpu.make_async_copy(before, u.at[1, pl.ds(1, J), pl.ds(1, I)], load_sem.at[3]),
        pltpu.make_async_copy(speed, cs, load_sem.at[4]),
    ]
    barrier = pltpu.get_barrier_semaphore()
    above, under_me = mx < nx - 1, mx > 0
    pairs = [(mx < nx - 1, x_side[0], mx > 0, x_side[1])]
    if nz > 1:
        pairs.append((mz < nz - 1, z_side[0], mz > 0, z_side[1]))
    if nz > 2:
        pairs.append((mz == 0, z_side[1], mz == nz - 1, z_side[0]))

    def greet(to):
        pl.semaphore_signal(barrier, inc=1, device_id=to, device_id_type=MESH)

    for d in range(1, ny):
        greet({"py": lax.rem(my + d, ny)})
    expected = ny - 1
    for has_upper, upper, has_lower, _ in pairs:
        @pl.when(has_upper)
        def _(upper=upper):
            greet(upper)

        expected = expected + jnp.where(has_lower, 1, 0)

    for load in loads[:2]:
        load.start()
    pl.semaphore_wait(barrier, expected)

    def meet():
        for n, (_, _, has_lower, lower) in enumerate(pairs):
            @pl.when(has_lower)
            def _(n=n, lower=lower):
                pl.semaphore_signal(ready.at[n], inc=1, device_id=lower, device_id_type=MESH)

        for n, (has_upper, _, _, _) in enumerate(pairs):
            @pl.when(has_upper)
            def _(n=n):
                pl.semaphore_wait(ready.at[n], 1)

    def hand_on():
        for way, (comes, goes) in enumerate(((under_me, above), (above, under_me))):
            @pl.when(comes)
            def _(way=way):
                pl.semaphore_wait(word.at[way], 1)

            @pl.when(goes)
            def _(way=way):
                pl.semaphore_signal(word.at[way], inc=1, device_id=x_side[way], device_id_type=MESH)

    def remote(src, dst, send, recv, to):
        return pltpu.make_async_remote_copy(
            src_ref=src, dst_ref=dst, send_sem=send, recv_sem=recv, device_id=to, device_id_type=MESH
        )

    def order(t):
        return (0, 1) if t % 2 == 0 else (1, 0)

    def cuts(t, side):
        return halves if t + 1 == STEPS and side == order(t)[1] else ((0, I),)

    def j_copy(t, side, c):
        row, rim = ((J - 1, 0), (0, J + 1))[side]
        start, size = cuts(t, side)[c]
        there = pl.ds(1 + start, size)
        return remote(u.at[t % 2, row + 1, there], u.at[t % 2, rim, there], x_send.at[t, side, c], x_recv.at[t, side, c], y_side[side])

    def i_copy(t, side, part):
        plane, rim = ((I - 1, 0), (0, I + 1))[side]
        start, size = parts[part]
        rows = pl.ds(start + 1, size)
        src = field.at[pl.ds(start, size), plane] if t == 0 else u.at[t % 2, rows, plane + 1]
        return remote(src, u.at[t % 2, rows, rim], z_send.at[t, side, part], z_recv.at[t, side, part], x_side[side])

    def k_copy(t, side, part):
        start, size = parts[part]
        rows = pl.ds(start, size)
        return remote(
            ysend.at[t, side, rows], yrecv.at[t, side, rows],
            y_send.at[t, side, part], y_recv.at[t, side, part], z_side[side],
        )

    def pack(t, j, i, value):
        ysend[t, 0, j, pl.ds(i, 1), :] = value[K - 1:K]
        ysend[t, 1, j, pl.ds(i, 1), :] = value[0:1]

    loads[0].wait()
    j_copy(0, 0, 0).start()
    loads[1].wait()
    j_copy(0, 1, 0).start()
    for load in loads[2:]:
        load.start()
    meet()
    hand_on()
    for part in range(3):
        for side in (0, 1):
            i_copy(0, side, part).start()

    loads[2].wait()

    def pack_row(j, carry):
        for i in range(I):
            ysend[0, 0, j, i:i + 1, :] = u[0, j + 1, i + 1, K - 1:K, :]
            ysend[0, 1, j, i:i + 1, :] = u[0, j + 1, i + 1, 0:1, :]
        return carry

    lax.fori_loop(0, J, pack_row, 0)
    for part in range(3):
        for side in (0, 1):
            k_copy(0, side, part).start()
    loads[3].wait()
    loads[4].wait()

    k_index = lax.broadcasted_iota(jnp.int32, (K, L), 0)

    def column(t, j, i):
        now, other = t % 2, (t + 1) % 2
        middle = u[now, j + 1, i + 1]
        low = jnp.where(k_index == 0, yrecv[t, 0, j, pl.ds(i, 1), :], pltpu.roll(middle, 1, 0))
        high = jnp.where(k_index == K - 1, yrecv[t, 1, j, pl.ds(i, 1), :], pltpu.roll(middle, K - 1, 0))
        spread = (
            u[now, j, i + 1] + u[now, j + 2, i + 1] + u[now, j + 1, i] + u[now, j + 1, i + 2]
            + low + high - 6.0 * middle
        )
        later = 2.0 * middle - u[other, j + 1, i + 1] + cs[j, i] * spread
        if t + 1 < STEPS:
            u[other, j + 1, i + 1] = later
            pack(t + 1, j, i, later)
        else:
            end[j, i] = later

    def total_copy(d, first):
        here = pl.ds(0, split if first else I)
        return remote(
            total.at[here], under.at[here] if d == 1 else below.at[d - 2, here], t_send.at[d - 1], t_recv.at[d - 1],
            {"py": lax.rem(my + d, ny)},
        )

    def for_totals(mine, first, act):
        for d in range(1, ny):
            @pl.when(jnp.logical_and(second_core if first else jnp.logical_not(second_core), my + d < ny if mine else my >= d))
            def _(d=d):
                act(total_copy(d, first), d)

    for t in range(STEPS):
        last = t + 1 == STEPS
        for side in (0, 1):
            i_copy(t, side, 0).wait_recv()
            k_copy(t, side, 0).wait_recv()
            if t > 0:
                i_copy(t - 1, side, 0).wait_send()

        def inner(q, carry, t=t):
            j = 1 + q // (I // 2)
            i = lax.rem(q, I // 2) * 2
            column(t, j, i)
            column(t, j, i + 1)
            return carry

        lax.fori_loop(0, (J - 2) * (I // 2), inner, 0)
        if not last:
            for side in (0, 1):
                i_copy(t + 1, side, 0).start()
                k_copy(t + 1, side, 0).start()

        for s in order(t):
            row, part = ((0, 1), (J - 1, 2))[s]
            for side in (0, 1):
                i_copy(t, side, part).wait_recv()
                k_copy(t, side, part).wait_recv()
                if t > 0:
                    i_copy(t - 1, side, part).wait_send()
            if t > 0:
                j_copy(t - 1, 1 - s, 0).wait_send()

            def outer(i, carry, t=t, row=row, s=s):
                column(t, row, i)
                if t + 1 == STEPS and s == order(t)[1]:
                    total[i] = total[i] + end[row, i]
                return carry

            if last and s == order(t)[1]:
                def add_up(i, carry, row=row):
                    value, *others = (end[j, i] for j in range(J) if j != row)
                    for other in others:
                        value = value + other
                    total[i] = value
                    return carry

                lax.fori_loop(0, I, add_up, 0)

            if not last:
                j_copy(t, s, 0).wait_recv()
                for c, (start, size) in enumerate(cuts(t + 1, 1 - s)):
                    lax.fori_loop(start, start + size, outer, 0)
                    j_copy(t + 1, 1 - s, c).start()
                for side in (0, 1):
                    i_copy(t + 1, side, part).start()
                    k_copy(t + 1, side, part).start()
            else:
                for c, (start, size) in enumerate(cuts(t, s)):
                    j_copy(t, s, c).wait_recv()
                    lax.fori_loop(start, start + size, outer, 0)
                    if s == order(t)[1]:
                        for_totals(True, c == 0, lambda copy, d: copy.start())

    @pl.when(my == 0)
    def _():
        under[...] = jnp.zeros((I, K, L), jnp.float32)

    for first in (True, False):
        def take(copy, d, size=split if first else I):
            copy.wait_recv()
            if d > 1:
                under[:size] = under[:size] + below[d - 2, :size]

        for_totals(False, first, take)

    for side in (0, 1):
        for c in range(len(cuts(STEPS - 1, side))):
            j_copy(STEPS - 1, side, c).wait_send()
        for part in range(3):
            i_copy(STEPS - 1, side, part).wait_send()
            for t in range(STEPS):
                k_copy(t, side, part).wait_send()
    for first in (True, False):
        for_totals(True, first, lambda copy, d: copy.wait_send())


def rest_kernel(ny, split, total, _, under_rest, below, send, recv):
    size = total.shape[0] - split
    my = lax.axis_index("py")
    there = pl.ds(split, size)
    second_core = lax.rem(lax.axis_index("pz"), 2) == 1

    def copy(d):
        return pltpu.make_async_remote_copy(
            src_ref=total.at[there], dst_ref=under_rest if d == 1 else below.at[d - 2],
            send_sem=send.at[d - 1], recv_sem=recv.at[d - 1],
            device_id={"py": lax.rem(my + d, ny)}, device_id_type=MESH,
        )

    @pl.when(my == 0)
    def _():
        under_rest[...] = jnp.zeros(under_rest.shape, jnp.float32)

    @pl.when(second_core)
    def _():
        barrier = pltpu.get_barrier_semaphore()
        for d in range(1, ny):
            @pl.when(my >= d)
            def _(d=d):
                pl.semaphore_signal(barrier, inc=1, device_id={"py": lax.rem(my + ny - d, ny)}, device_id_type=MESH)

        @pl.when(my < ny - 1)
        def _():
            pl.semaphore_wait(barrier, ny - 1 - my)

        for d in range(1, ny):
            @pl.when(my + d < ny)
            def _(d=d):
                copy(d).start()

        for d in range(1, ny):
            @pl.when(my >= d)
            def _(d=d):
                copy(d).wait_recv()
                if d > 1:
                    under_rest[...] = under_rest[...] + below[d - 2]

        for d in range(1, ny):
            @pl.when(my + d < ny)
            def _(d=d):
                copy(d).wait_send()


def columns_out(scale, start, size, end, under, sums_out, csum, sem):
    J = end.shape[0]
    chunks = max(n for n in range(1, OUT_CHUNKS + 1) if size % n == 0)
    width = size // chunks

    def sum_copy(c):
        here = pl.ds(c * width, width)
        return pltpu.make_async_copy(csum.at[:, here], sums_out.at[:, pl.ds(start + c * width, width)], sem.at[c])

    for c in range(chunks):
        def running(i, carry):
            value = under[i]
            for j in range(J):
                value = value + end[j, start + i]
                csum[j, i] = value * scale
            return carry

        lax.fori_loop(c * width, (c + 1) * width, running, 0)
        sum_copy(c).start()
    return [sum_copy(c) for c in range(chunks)]


def first_out_kernel(scale, split, end, under, sums_out, field_out, done, csum, sem, field_sem):
    whole = pltpu.make_async_copy(end, field_out, field_sem)
    whole.start()
    second_core = lax.rem(lax.axis_index("pz"), 2) == 1

    def columns(size):
        for copy in columns_out(scale, 0, size, end, under, sums_out, csum, sem):
            copy.wait()

    @pl.when(second_core)
    def _():
        columns(split)

    @pl.when(jnp.logical_not(second_core))
    def _():
        columns(end.shape[1])

    whole.wait()
    done[...] = jnp.zeros(done.shape, jnp.float32)


def rest_out_kernel(scale, split, end, under_rest, _, sums_out, csum, sem):
    @pl.when(lax.rem(lax.axis_index("pz"), 2) == 1)
    def _():
        for copy in columns_out(scale, split, end.shape[1] - split, end, under_rest, sums_out, csum, sem):
            copy.wait()


def local(peers, field_now, earlier, speed_square):
    J, I, K, L = field_now.shape
    ny = peers[0]
    split = I * FIRST[0] // FIRST[1]
    f32 = jnp.float32
    dma = pltpu.SemaphoreType.DMA
    anywhere = pl.BlockSpec(memory_space=pltpu.MemorySpace.HBM)
    shape = jax.ShapeDtypeStruct(field_now.shape, f32)
    slots, extra = max(ny - 1, 1), max(ny - 2, 1)
    resident = pl.BlockSpec(memory_space=pltpu.VMEM)
    end, under, total = pl.pallas_call(
        functools.partial(march_kernel, peers, split),
        out_shape=(pltpu.VMEM((J, I, K, L), f32), pltpu.VMEM((I, K, L), f32), pltpu.VMEM((I, K, L), f32)),
        in_specs=[anywhere] * 3,
        out_specs=(resident,) * 3,
        scratch_shapes=[
            pltpu.VMEM((2, J + 2, I + 2, K, L), f32),
            pltpu.VMEM((J, I, K, L), f32),
            pltpu.VMEM((extra, I, K, L), f32),
            pltpu.VMEM((STEPS, 2, J, I, L), f32),
            pltpu.VMEM((STEPS, 2, J, I, L), f32),
            dma((5,)),
            dma((STEPS, 2, 2)),
            dma((STEPS, 2, 2)),
            dma((STEPS, 2, 3)),
            dma((STEPS, 2, 3)),
            dma((STEPS, 2, 3)),
            dma((STEPS, 2, 3)),
            dma((slots,)),
            dma((slots,)),
            pltpu.SemaphoreType.REGULAR((2,)),
            pltpu.SemaphoreType.REGULAR((3,)),
        ],
        compiler_params=pltpu.CompilerParams(
            collective_id=0, has_side_effects=True, vmem_limit_bytes=56 * 1024 * 1024
        ),
        name="march",
    )(field_now, earlier, speed_square)
    scale = 1.0 / (J * ny)
    small = pltpu.CompilerParams(vmem_limit_bytes=16 * 1024 * 1024)

    sums, field_end, done = pl.pallas_call(
        functools.partial(first_out_kernel, scale, split),
        out_shape=(shape, shape, pltpu.VMEM((8, L), f32)),
        in_specs=[resident] * 2,
        out_specs=(anywhere, anywhere, resident),
        scratch_shapes=[pltpu.VMEM((J, I, K, L), f32), dma((OUT_CHUNKS,)), dma],
        compiler_params=small,
        name="first_out",
    )(end, under)
    rest = I - split
    under_rest = pl.pallas_call(
        functools.partial(rest_kernel, ny, split),
        out_shape=pltpu.VMEM((rest, K, L), f32),
        in_specs=[resident] * 2,
        out_specs=resident,
        scratch_shapes=[pltpu.VMEM((extra, rest, K, L), f32), dma((slots,)), dma((slots,))],
        compiler_params=pltpu.CompilerParams(
            collective_id=1, has_side_effects=True, vmem_limit_bytes=16 * 1024 * 1024
        ),
        name="rest",
    )(total, done)
    sums = pl.pallas_call(
        functools.partial(rest_out_kernel, scale, split),
        out_shape=shape,
        in_specs=[resident] * 2 + [anywhere],
        out_specs=anywhere,
        input_output_aliases={2: 0},
        scratch_shapes=[pltpu.VMEM((J, rest, K, L), f32), dma((OUT_CHUNKS,))],
        compiler_params=small,
        name="rest_out",
    )(end, under_rest, sums)
    return sums, field_end


def solution(mesh):
    placed = P("py", "px", "pz", None)
    peers = tuple(mesh.shape[a] for a in ("py", "px", "pz"))
    return jax.shard_map(
        functools.partial(local, peers),
        mesh=mesh,
        in_specs=(placed,) * 3,
        out_specs=(placed,) * 2,
        check_vma=False,
    )
```

```python
import functools

import jax
import jax.numpy as jnp
from jax import lax
from jax.experimental import pallas as pl
from jax.experimental.pallas import tpu as pltpu
from jax.sharding import PartitionSpec as P

STEPS = 4
OUT_CHUNKS = 4
FIRST = (7, 16)
MESH = pl.DeviceIdType.MESH


def march_kernel(
    peers, split, field, before, speed, end, under, total,
    u, cs, below, ysend, yrecv,
    load_sem, x_send, x_recv, z_send, z_recv, y_send, y_recv, t_send, t_recv, word, ready,
):
    J, I, K, L = field.shape
    ny, nx, nz = peers
    my, mx, mz = (lax.axis_index(a) for a in ("py", "px", "pz"))
    y_side = ({"py": lax.rem(my + 1, ny)}, {"py": lax.rem(my + ny - 1, ny)})
    x_side = ({"px": lax.rem(mx + 1, nx)}, {"px": lax.rem(mx + nx - 1, nx)})
    z_side = ({"pz": lax.rem(mz + 1, nz)}, {"pz": lax.rem(mz + nz - 1, nz)})
    parts = ((1, J - 2), (0, 1), (J - 1, 1))
    near = I - max(I // 16, 1)
    cut = ((0, split), (split, near - split), (near, I - near))
    sent = ((0, split), (0, near), (near, I - near))
    second_core = lax.rem(mz, 2) == 1

    loads = [
        pltpu.make_async_copy(
            field.at[pl.ds(start, size)], u.at[0, pl.ds(start + 1, size), pl.ds(1, I)], load_sem.at[part]
        )
        for part, (start, size) in reversed(tuple(enumerate(parts)))
    ] + [
        pltpu.make_async_copy(before, u.at[1, pl.ds(1, J), pl.ds(1, I)], load_sem.at[3]),
        pltpu.make_async_copy(speed, cs, load_sem.at[4]),
    ]
    barrier = pltpu.get_barrier_semaphore()
    above, under_me = mx < nx - 1, mx > 0
    pairs = [(mx < nx - 1, x_side[0], mx > 0, x_side[1])]
    if nz > 1:
        pairs.append((mz < nz - 1, z_side[0], mz > 0, z_side[1]))
    if nz > 2:
        pairs.append((mz == 0, z_side[1], mz == nz - 1, z_side[0]))

    def greet(to):
        pl.semaphore_signal(barrier, inc=1, device_id=to, device_id_type=MESH)

    for d in range(1, ny):
        greet({"py": lax.rem(my + d, ny)})
    expected = ny - 1
    for has_upper, upper, has_lower, _ in pairs:
        @pl.when(has_upper)
        def _(upper=upper):
            greet(upper)

        expected = expected + jnp.where(has_lower, 1, 0)

    for load in loads[:2]:
        load.start()
    pl.semaphore_wait(barrier, expected)

    def meet():
        for n, (_, _, has_lower, lower) in enumerate(pairs):
            @pl.when(has_lower)
            def _(n=n, lower=lower):
                pl.semaphore_signal(ready.at[n], inc=1, device_id=lower, device_id_type=MESH)

        for n, (has_upper, _, _, _) in enumerate(pairs):
            @pl.when(has_upper)
            def _(n=n):
                pl.semaphore_wait(ready.at[n], 1)

    def hand_on():
        for way, (comes, goes) in enumerate(((under_me, above), (above, under_me))):
            @pl.when(comes)
            def _(way=way):
                pl.semaphore_wait(word.at[way], 1)

            @pl.when(goes)
            def _(way=way):
                pl.semaphore_signal(word.at[way], inc=1, device_id=x_side[way], device_id_type=MESH)

    def remote(src, dst, send, recv, to):
        return pltpu.make_async_remote_copy(
            src_ref=src, dst_ref=dst, send_sem=send, recv_sem=recv, device_id=to, device_id_type=MESH
        )

    def order(t):
        return (0, 1) if t % 2 == 0 else (1, 0)

    def cuts(t, side):
        return cut if t + 1 == STEPS and side == order(t)[1] else ((0, I),)

    def j_copy(t, side, c):
        row, rim = ((J - 1, 0), (0, J + 1))[side]
        start, size = cuts(t, side)[c]
        there = pl.ds(1 + start, size)
        return remote(u.at[t % 2, row + 1, there], u.at[t % 2, rim, there], x_send.at[t, side, c], x_recv.at[t, side, c], y_side[side])

    def i_copy(t, side, part):
        plane, rim = ((I - 1, 0), (0, I + 1))[side]
        start, size = parts[part]
        rows = pl.ds(start + 1, size)
        src = field.at[pl.ds(start, size), plane] if t == 0 else u.at[t % 2, rows, plane + 1]
        return remote(src, u.at[t % 2, rows, rim], z_send.at[t, side, part], z_recv.at[t, side, part], x_side[side])

    def k_copy(t, side, part):
        start, size = parts[part]
        rows = pl.ds(start, size)
        return remote(
            ysend.at[t, side, rows], yrecv.at[t, side, rows],
            y_send.at[t, side, part], y_recv.at[t, side, part], z_side[side],
        )

    def pack(t, j, i, value):
        ysend[t, 0, j, pl.ds(i, 1), :] = value[K - 1:K]
        ysend[t, 1, j, pl.ds(i, 1), :] = value[0:1]

    loads[0].wait()
    j_copy(0, 0, 0).start()
    loads[1].wait()
    j_copy(0, 1, 0).start()
    for load in loads[2:]:
        load.start()
    meet()
    hand_on()
    for part in range(3):
        for side in (0, 1):
            i_copy(0, side, part).start()

    loads[2].wait()

    def pack_row(j, carry):
        for i in range(I):
            ysend[0, 0, j, i:i + 1, :] = u[0, j + 1, i + 1, K - 1:K, :]
            ysend[0, 1, j, i:i + 1, :] = u[0, j + 1, i + 1, 0:1, :]
        return carry

    lax.fori_loop(0, J, pack_row, 0)
    for part in range(3):
        for side in (0, 1):
            k_copy(0, side, part).start()
    loads[3].wait()
    loads[4].wait()

    k_index = lax.broadcasted_iota(jnp.int32, (K, L), 0)

    def column(t, j, i):
        now, other = t % 2, (t + 1) % 2
        middle = u[now, j + 1, i + 1]
        low = jnp.where(k_index == 0, yrecv[t, 0, j, pl.ds(i, 1), :], pltpu.roll(middle, 1, 0))
        high = jnp.where(k_index == K - 1, yrecv[t, 1, j, pl.ds(i, 1), :], pltpu.roll(middle, K - 1, 0))
        spread = (
            u[now, j, i + 1] + u[now, j + 2, i + 1] + u[now, j + 1, i] + u[now, j + 1, i + 2]
            + low + high - 6.0 * middle
        )
        later = 2.0 * middle - u[other, j + 1, i + 1] + cs[j, i] * spread
        if t + 1 < STEPS:
            u[other, j + 1, i + 1] = later
            pack(t + 1, j, i, later)
        else:
            end[j, i] = later

    def total_copy(d, c):
        here = pl.ds(*sent[c])
        return remote(
            total.at[here], under.at[here] if d == 1 else below.at[d - 2, here], t_send.at[d - 1, c], t_recv.at[d - 1, c],
            {"py": lax.rem(my + d, ny)},
        )

    def for_totals(mine, c, act):
        for d in range(1, ny):
            @pl.when(jnp.logical_and(second_core if c == 0 else jnp.logical_not(second_core), my + d < ny if mine else my >= d))
            def _(d=d):
                act(total_copy(d, c), d)

    for t in range(STEPS):
        last = t + 1 == STEPS
        for side in (0, 1):
            i_copy(t, side, 0).wait_recv()
            k_copy(t, side, 0).wait_recv()
            if t > 0:
                i_copy(t - 1, side, 0).wait_send()

        def inner(q, carry, t=t):
            j = 1 + q // (I // 2)
            i = lax.rem(q, I // 2) * 2
            column(t, j, i)
            column(t, j, i + 1)
            return carry

        lax.fori_loop(0, (J - 2) * (I // 2), inner, 0)
        if not last:
            for side in (0, 1):
                i_copy(t + 1, side, 0).start()
                k_copy(t + 1, side, 0).start()

        for s in order(t):
            row, part = ((0, 1), (J - 1, 2))[s]
            for side in (0, 1):
                i_copy(t, side, part).wait_recv()
                k_copy(t, side, part).wait_recv()
                if t > 0:
                    i_copy(t - 1, side, part).wait_send()
            if t > 0:
                j_copy(t - 1, 1 - s, 0).wait_send()

            def outer(i, carry, t=t, row=row, s=s):
                column(t, row, i)
                if t + 1 == STEPS and s == order(t)[1]:
                    total[i] = total[i] + end[row, i]
                return carry

            if last and s == order(t)[1]:
                def add_up(i, carry, row=row):
                    value, *others = (end[j, i] for j in range(J) if j != row)
                    for other in others:
                        value = value + other
                    total[i] = value
                    return carry

                lax.fori_loop(0, I, add_up, 0)

            if not last:
                j_copy(t, s, 0).wait_recv()
                for c, (start, size) in enumerate(cuts(t + 1, 1 - s)):
                    lax.fori_loop(start, start + size, outer, 0)
                    j_copy(t + 1, 1 - s, c).start()
                for side in (0, 1):
                    i_copy(t + 1, side, part).start()
                    k_copy(t + 1, side, part).start()
            else:
                for c, (start, size) in enumerate(cuts(t, s)):
                    j_copy(t, s, c).wait_recv()
                    lax.fori_loop(start, start + size, outer, 0)
                    if s == order(t)[1]:
                        for_totals(True, c, lambda copy, d: copy.start())

    @pl.when(my == 0)
    def _():
        under[...] = jnp.zeros((I, K, L), jnp.float32)

    for c, (start, size) in enumerate(sent):
        def take(copy, d, here=pl.ds(start, size)):
            copy.wait_recv()
            if d > 1:
                under[here] = under[here] + below[d - 2, here]

        for_totals(False, c, take)

    for side in (0, 1):
        for c in range(len(cuts(STEPS - 1, side))):
            j_copy(STEPS - 1, side, c).wait_send()
        for part in range(3):
            i_copy(STEPS - 1, side, part).wait_send()
            for t in range(STEPS):
                k_copy(t, side, part).wait_send()
    for c in range(len(sent)):
        for_totals(True, c, lambda copy, d: copy.wait_send())


def rest_kernel(ny, split, total, _, under_rest, below, send, recv):
    size = total.shape[0] - split
    my = lax.axis_index("py")
    there = pl.ds(split, size)
    second_core = lax.rem(lax.axis_index("pz"), 2) == 1

    def copy(d):
        return pltpu.make_async_remote_copy(
            src_ref=total.at[there], dst_ref=under_rest if d == 1 else below.at[d - 2],
            send_sem=send.at[d - 1], recv_sem=recv.at[d - 1],
            device_id={"py": lax.rem(my + d, ny)}, device_id_type=MESH,
        )

    @pl.when(my == 0)
    def _():
        under_rest[...] = jnp.zeros(under_rest.shape, jnp.float32)

    @pl.when(second_core)
    def _():
        barrier = pltpu.get_barrier_semaphore()
        for d in range(1, ny):
            @pl.when(my >= d)
            def _(d=d):
                pl.semaphore_signal(barrier, inc=1, device_id={"py": lax.rem(my + ny - d, ny)}, device_id_type=MESH)

        @pl.when(my < ny - 1)
        def _():
            pl.semaphore_wait(barrier, ny - 1 - my)

        for d in range(1, ny):
            @pl.when(my + d < ny)
            def _(d=d):
                copy(d).start()

        for d in range(1, ny):
            @pl.when(my >= d)
            def _(d=d):
                copy(d).wait_recv()
                if d > 1:
                    under_rest[...] = under_rest[...] + below[d - 2]

        for d in range(1, ny):
            @pl.when(my + d < ny)
            def _(d=d):
                copy(d).wait_send()


def columns_out(scale, start, size, end, under, sums_out, csum, sem):
    J = end.shape[0]
    pieces = min(OUT_CHUNKS, size) - 1
    bounds = [0] + [1 + (size - 1) * n // max(pieces, 1) for n in range(pieces + 1)]

    def sum_copy(c):
        low, width = bounds[c], bounds[c + 1] - bounds[c]
        return pltpu.make_async_copy(
            csum.at[:, pl.ds(low, width)], sums_out.at[:, pl.ds(start + low, width)], sem.at[c]
        )

    for c in range(pieces + 1):
        def running(i, carry):
            value = under[i]
            for j in range(J):
                value = value + end[j, start + i]
                csum[j, i] = value * scale
            return carry

        lax.fori_loop(bounds[c], bounds[c + 1], running, 0)
        sum_copy(c).start()
    return [sum_copy(c) for c in range(pieces + 1)]


def first_out_kernel(scale, split, end, under, sums_out, field_out, done, csum, sem, field_sem):
    whole = pltpu.make_async_copy(end, field_out, field_sem)
    whole.start()
    second_core = lax.rem(lax.axis_index("pz"), 2) == 1

    def columns(size):
        for copy in columns_out(scale, 0, size, end, under, sums_out, csum, sem):
            copy.wait()

    @pl.when(second_core)
    def _():
        columns(split)

    @pl.when(jnp.logical_not(second_core))
    def _():
        columns(end.shape[1])

    whole.wait()
    done[...] = jnp.zeros(done.shape, jnp.float32)


def rest_out_kernel(scale, split, end, under_rest, _, sums_out, csum, sem):
    @pl.when(lax.rem(lax.axis_index("pz"), 2) == 1)
    def _():
        for copy in columns_out(scale, split, end.shape[1] - split, end, under_rest, sums_out, csum, sem):
            copy.wait()


def local(peers, field_now, earlier, speed_square):
    J, I, K, L = field_now.shape
    ny = peers[0]
    split = I * FIRST[0] // FIRST[1]
    f32 = jnp.float32
    dma = pltpu.SemaphoreType.DMA
    anywhere = pl.BlockSpec(memory_space=pltpu.MemorySpace.HBM)
    shape = jax.ShapeDtypeStruct(field_now.shape, f32)
    slots, extra = max(ny - 1, 1), max(ny - 2, 1)
    resident = pl.BlockSpec(memory_space=pltpu.VMEM)
    end, under, total = pl.pallas_call(
        functools.partial(march_kernel, peers, split),
        out_shape=(pltpu.VMEM((J, I, K, L), f32), pltpu.VMEM((I, K, L), f32), pltpu.VMEM((I, K, L), f32)),
        in_specs=[anywhere] * 3,
        out_specs=(resident,) * 3,
        scratch_shapes=[
            pltpu.VMEM((2, J + 2, I + 2, K, L), f32),
            pltpu.VMEM((J, I, K, L), f32),
            pltpu.VMEM((extra, I, K, L), f32),
            pltpu.VMEM((STEPS, 2, J, I, L), f32),
            pltpu.VMEM((STEPS, 2, J, I, L), f32),
            dma((5,)),
            dma((STEPS, 2, 3)),
            dma((STEPS, 2, 3)),
            dma((STEPS, 2, 3)),
            dma((STEPS, 2, 3)),
            dma((STEPS, 2, 3)),
            dma((STEPS, 2, 3)),
            dma((slots, 3)),
            dma((slots, 3)),
            pltpu.SemaphoreType.REGULAR((2,)),
            pltpu.SemaphoreType.REGULAR((3,)),
        ],
        compiler_params=pltpu.CompilerParams(
            collective_id=0, has_side_effects=True, vmem_limit_bytes=56 * 1024 * 1024
        ),
        name="march",
    )(field_now, earlier, speed_square)
    scale = 1.0 / (J * ny)
    small = pltpu.CompilerParams(vmem_limit_bytes=16 * 1024 * 1024)

    sums, field_end, done = pl.pallas_call(
        functools.partial(first_out_kernel, scale, split),
        out_shape=(shape, shape, pltpu.VMEM((8, L), f32)),
        in_specs=[resident] * 2,
        out_specs=(anywhere, anywhere, resident),
        scratch_shapes=[pltpu.VMEM((J, I, K, L), f32), dma((OUT_CHUNKS,)), dma],
        compiler_params=small,
        name="first_out",
    )(end, under)
    rest = I - split
    under_rest = pl.pallas_call(
        functools.partial(rest_kernel, ny, split),
        out_shape=pltpu.VMEM((rest, K, L), f32),
        in_specs=[resident] * 2,
        out_specs=resident,
        scratch_shapes=[pltpu.VMEM((extra, rest, K, L), f32), dma((slots,)), dma((slots,))],
        compiler_params=pltpu.CompilerParams(
            collective_id=1, has_side_effects=True, vmem_limit_bytes=16 * 1024 * 1024
        ),
        name="rest",
    )(total, done)
    sums = pl.pallas_call(
        functools.partial(rest_out_kernel, scale, split),
        out_shape=shape,
        in_specs=[resident] * 2 + [anywhere],
        out_specs=anywhere,
        input_output_aliases={2: 0},
        scratch_shapes=[pltpu.VMEM((J, rest, K, L), f32), dma((OUT_CHUNKS,))],
        compiler_params=small,
        name="rest_out",
    )(end, under_rest, sums)
    return sums, field_end


def solution(mesh):
    placed = P("py", "px", "pz", None)
    peers = tuple(mesh.shape[a] for a in ("py", "px", "pz"))
    return jax.shard_map(
        functools.partial(local, peers),
        mesh=mesh,
        in_specs=(placed,) * 3,
        out_specs=(placed,) * 2,
        check_vma=False,
    )
```

```python
import functools

import jax
import jax.numpy as jnp
from jax import lax
from jax.experimental import pallas as pl
from jax.experimental.pallas import tpu as pltpu
from jax.sharding import PartitionSpec as P

STEPS = 4
OUT_CHUNKS = 4
FIRST = (1, 2)
MESH = pl.DeviceIdType.MESH


def march_kernel(
    peers, split, field, before, speed, end, under, total,
    u, cs, below, ysend, yrecv,
    load_sem, x_send, x_recv, z_send, z_recv, y_send, y_recv, t_send, t_recv, word, ready,
):
    J, I, K, L = field.shape
    ny, nx, nz = peers
    my, mx, mz = (lax.axis_index(a) for a in ("py", "px", "pz"))
    y_side = ({"py": lax.rem(my + 1, ny)}, {"py": lax.rem(my + ny - 1, ny)})
    x_side = ({"px": lax.rem(mx + 1, nx)}, {"px": lax.rem(mx + nx - 1, nx)})
    z_side = ({"pz": lax.rem(mz + 1, nz)}, {"pz": lax.rem(mz + nz - 1, nz)})
    parts = ((1, J - 2), (0, 1), (J - 1, 1))
    halves = ((0, split), (split, I - split))
    second_core = lax.rem(mz, 2) == 1

    loads = [
        pltpu.make_async_copy(
            field.at[pl.ds(start, size)], u.at[0, pl.ds(start + 1, size), pl.ds(1, I)], load_sem.at[part]
        )
        for part, (start, size) in reversed(tuple(enumerate(parts)))
    ] + [
        pltpu.make_async_copy(before, u.at[1, pl.ds(1, J), pl.ds(1, I)], load_sem.at[3]),
        pltpu.make_async_copy(speed, cs, load_sem.at[4]),
    ]
    barrier = pltpu.get_barrier_semaphore()
    above, under_me = mx < nx - 1, mx > 0
    pairs = [(mx < nx - 1, x_side[0], mx > 0, x_side[1])]
    if nz > 1:
        pairs.append((mz < nz - 1, z_side[0], mz > 0, z_side[1]))
    if nz > 2:
        pairs.append((mz == 0, z_side[1], mz == nz - 1, z_side[0]))

    def greet(to):
        pl.semaphore_signal(barrier, inc=1, device_id=to, device_id_type=MESH)

    for d in range(1, ny):
        greet({"py": lax.rem(my + d, ny)})
    expected = ny - 1
    for has_upper, upper, has_lower, _ in pairs:
        @pl.when(has_upper)
        def _(upper=upper):
            greet(upper)

        expected = expected + jnp.where(has_lower, 1, 0)

    for load in loads[:2]:
        load.start()
    pl.semaphore_wait(barrier, expected)

    def meet():
        for n, (_, _, has_lower, lower) in enumerate(pairs):
            @pl.when(has_lower)
            def _(n=n, lower=lower):
                pl.semaphore_signal(ready.at[n], inc=1, device_id=lower, device_id_type=MESH)

        for n, (has_upper, _, _, _) in enumerate(pairs):
            @pl.when(has_upper)
            def _(n=n):
                pl.semaphore_wait(ready.at[n], 1)

    def hand_on():
        for way, (comes, goes) in enumerate(((under_me, above), (above, under_me))):
            @pl.when(comes)
            def _(way=way):
                pl.semaphore_wait(word.at[way], 1)

            @pl.when(goes)
            def _(way=way):
                pl.semaphore_signal(word.at[way], inc=1, device_id=x_side[way], device_id_type=MESH)

    def remote(src, dst, send, recv, to):
        return pltpu.make_async_remote_copy(
            src_ref=src, dst_ref=dst, send_sem=send, recv_sem=recv, device_id=to, device_id_type=MESH
        )

    def order(t):
        return (0, 1) if t % 2 == 0 else (1, 0)

    def cuts(t, side):
        return halves if t + 1 == STEPS and side == order(t)[1] else ((0, I),)

    def j_copy(t, side, c):
        row, rim = ((J - 1, 0), (0, J + 1))[side]
        start, size = cuts(t, side)[c]
        there = pl.ds(1 + start, size)
        return remote(u.at[t % 2, row + 1, there], u.at[t % 2, rim, there], x_send.at[t, side, c], x_recv.at[t, side, c], y_side[side])

    def i_copy(t, side, part):
        plane, rim = ((I - 1, 0), (0, I + 1))[side]
        start, size = parts[part]
        rows = pl.ds(start + 1, size)
        src = field.at[pl.ds(start, size), plane] if t == 0 else u.at[t % 2, rows, plane + 1]
        return remote(src, u.at[t % 2, rows, rim], z_send.at[t, side, part], z_recv.at[t, side, part], x_side[side])

    def k_copy(t, side, part):
        start, size = parts[part]
        rows = pl.ds(start, size)
        return remote(
            ysend.at[t, side, rows], yrecv.at[t, side, rows],
            y_send.at[t, side, part], y_recv.at[t, side, part], z_side[side],
        )

    def pack(t, j, i, value):
        ysend[t, 0, j, pl.ds(i, 1), :] = value[K - 1:K]
        ysend[t, 1, j, pl.ds(i, 1), :] = value[0:1]

    loads[0].wait()
    j_copy(0, 0, 0).start()
    loads[1].wait()
    j_copy(0, 1, 0).start()
    for load in loads[2:]:
        load.start()
    meet()
    hand_on()
    for part in range(3):
        for side in (0, 1):
            i_copy(0, side, part).start()

    loads[2].wait()

    def pack_row(j, carry):
        for i in range(I):
            ysend[0, 0, j, i:i + 1, :] = u[0, j + 1, i + 1, K - 1:K, :]
            ysend[0, 1, j, i:i + 1, :] = u[0, j + 1, i + 1, 0:1, :]
        return carry

    lax.fori_loop(0, J, pack_row, 0)
    for part in range(3):
        for side in (0, 1):
            k_copy(0, side, part).start()
    loads[3].wait()
    loads[4].wait()

    k_index = lax.broadcasted_iota(jnp.int32, (K, L), 0)

    def column(t, j, i):
        now, other = t % 2, (t + 1) % 2
        middle = u[now, j + 1, i + 1]
        low = jnp.where(k_index == 0, yrecv[t, 0, j, pl.ds(i, 1), :], pltpu.roll(middle, 1, 0))
        high = jnp.where(k_index == K - 1, yrecv[t, 1, j, pl.ds(i, 1), :], pltpu.roll(middle, K - 1, 0))
        spread = (
            u[now, j, i + 1] + u[now, j + 2, i + 1] + u[now, j + 1, i] + u[now, j + 1, i + 2]
            + low + high - 6.0 * middle
        )
        later = 2.0 * middle - u[other, j + 1, i + 1] + cs[j, i] * spread
        if t + 1 < STEPS:
            u[other, j + 1, i + 1] = later
            pack(t + 1, j, i, later)
        else:
            end[j, i] = later

    def total_copy(d, first):
        here = pl.ds(0, split if first else I)
        return remote(
            total.at[here], below.at[d - 1, here], t_send.at[d - 1], t_recv.at[d - 1], {"py": lax.rem(my + d, ny)}
        )

    def for_totals(mine, first, act):
        for d in range(1, ny):
            @pl.when(jnp.logical_and(second_core if first else jnp.logical_not(second_core), my + d < ny if mine else my >= d))
            def _(d=d):
                act(total_copy(d, first), d)

    for t in range(STEPS):
        last = t + 1 == STEPS
        for side in (0, 1):
            i_copy(t, side, 0).wait_recv()
            k_copy(t, side, 0).wait_recv()
            if t > 0:
                i_copy(t - 1, side, 0).wait_send()

        def inner(q, carry, t=t):
            j = 1 + q // (I // 2)
            i = lax.rem(q, I // 2) * 2
            column(t, j, i)
            column(t, j, i + 1)
            return carry

        lax.fori_loop(0, (J - 2) * (I // 2), inner, 0)
        if not last:
            for side in (0, 1):
                i_copy(t + 1, side, 0).start()
                k_copy(t + 1, side, 0).start()

        for s in order(t):
            row, part = ((0, 1), (J - 1, 2))[s]
            for side in (0, 1):
                i_copy(t, side, part).wait_recv()
                k_copy(t, side, part).wait_recv()
                if t > 0:
                    i_copy(t - 1, side, part).wait_send()
            if t > 0:
                j_copy(t - 1, 1 - s, 0).wait_send()

            def outer(i, carry, t=t, row=row, s=s):
                column(t, row, i)
                if t + 1 == STEPS and s == order(t)[1]:
                    total[i] = total[i] + end[row, i]
                return carry

            if last and s == order(t)[1]:
                def add_up(i, carry, row=row):
                    value, *others = (end[j, i] for j in range(J) if j != row)
                    for other in others:
                        value = value + other
                    total[i] = value
                    return carry

                lax.fori_loop(0, I, add_up, 0)

            if not last:
                j_copy(t, s, 0).wait_recv()
                for c, (start, size) in enumerate(cuts(t + 1, 1 - s)):
                    lax.fori_loop(start, start + size, outer, 0)
                    j_copy(t + 1, 1 - s, c).start()
                for side in (0, 1):
                    i_copy(t + 1, side, part).start()
                    k_copy(t + 1, side, part).start()
            else:
                for c, (start, size) in enumerate(cuts(t, s)):
                    j_copy(t, s, c).wait_recv()
                    lax.fori_loop(start, start + size, outer, 0)
                    if s == order(t)[1]:
                        for_totals(True, c == 0, lambda copy, d: copy.start())

    under[...] = jnp.zeros((I, K, L), jnp.float32)
    for first in (True, False):
        def take(copy, d, size=split if first else I):
            copy.wait_recv()
            under[:size] = under[:size] + below[d - 1, :size]

        for_totals(False, first, take)

    for side in (0, 1):
        for c in range(len(cuts(STEPS - 1, side))):
            j_copy(STEPS - 1, side, c).wait_send()
        for part in range(3):
            i_copy(STEPS - 1, side, part).wait_send()
            for t in range(STEPS):
                k_copy(t, side, part).wait_send()
    for first in (True, False):
        for_totals(True, first, lambda copy, d: copy.wait_send())


def rest_kernel(ny, split, total, under, _, under_rest, below, send, recv):
    size = total.shape[0] - split
    my = lax.axis_index("py")
    there = pl.ds(split, size)
    second_core = lax.rem(lax.axis_index("pz"), 2) == 1

    def copy(d):
        return pltpu.make_async_remote_copy(
            src_ref=total.at[there], dst_ref=below.at[d - 1], send_sem=send.at[d - 1], recv_sem=recv.at[d - 1],
            device_id={"py": lax.rem(my + d, ny)}, device_id_type=MESH,
        )

    under_rest[...] = under[split:]

    @pl.when(second_core)
    def _():
        barrier = pltpu.get_barrier_semaphore()
        for d in range(1, ny):
            @pl.when(my >= d)
            def _(d=d):
                pl.semaphore_signal(barrier, inc=1, device_id={"py": lax.rem(my + ny - d, ny)}, device_id_type=MESH)

        @pl.when(my < ny - 1)
        def _():
            pl.semaphore_wait(barrier, ny - 1 - my)

        for d in range(1, ny):
            @pl.when(my + d < ny)
            def _(d=d):
                copy(d).start()

        for d in range(1, ny):
            @pl.when(my >= d)
            def _(d=d):
                copy(d).wait_recv()
                under_rest[...] = under_rest[...] + below[d - 1]

        for d in range(1, ny):
            @pl.when(my + d < ny)
            def _(d=d):
                copy(d).wait_send()


def columns_out(scale, chunks, start, size, end, under, sums_out, csum, sem):
    J = end.shape[0]
    width = size // chunks

    def sum_copy(c):
        here = pl.ds(c * width, width)
        return pltpu.make_async_copy(csum.at[:, here], sums_out.at[:, pl.ds(start + c * width, width)], sem.at[c])

    for c in range(chunks):
        def running(i, carry):
            value = under[i]
            for j in range(J):
                value = value + end[j, start + i]
                csum[j, i] = value * scale
            return carry

        lax.fori_loop(c * width, (c + 1) * width, running, 0)
        sum_copy(c).start()
    return [sum_copy(c) for c in range(chunks)]


def first_out_kernel(scale, chunks, split, end, under, sums_out, field_out, done, csum, sem, field_sem):
    whole = pltpu.make_async_copy(end, field_out, field_sem)
    whole.start()
    partly = jnp.logical_and(lax.rem(lax.axis_index("pz"), 2) == 1, lax.axis_index("py") > 0)

    def columns(size):
        for copy in columns_out(scale, chunks, 0, size, end, under, sums_out, csum, sem):
            copy.wait()

    @pl.when(partly)
    def _():
        columns(split)

    @pl.when(jnp.logical_not(partly))
    def _():
        columns(end.shape[1])

    whole.wait()
    done[...] = jnp.zeros(done.shape, jnp.float32)


def rest_out_kernel(scale, chunks, split, end, under_rest, _, sums_out, csum, sem):
    @pl.when(jnp.logical_and(lax.rem(lax.axis_index("pz"), 2) == 1, lax.axis_index("py") > 0))
    def _():
        for copy in columns_out(scale, chunks, split, end.shape[1] - split, end, under_rest, sums_out, csum, sem):
            copy.wait()


def local(peers, field_now, earlier, speed_square):
    J, I, K, L = field_now.shape
    ny = peers[0]
    split = I * FIRST[0] // FIRST[1]
    f32 = jnp.float32
    dma = pltpu.SemaphoreType.DMA
    anywhere = pl.BlockSpec(memory_space=pltpu.MemorySpace.HBM)
    shape = jax.ShapeDtypeStruct(field_now.shape, f32)
    slots = max(ny - 1, 1)
    resident = pl.BlockSpec(memory_space=pltpu.VMEM)
    end, under, total = pl.pallas_call(
        functools.partial(march_kernel, peers, split),
        out_shape=(pltpu.VMEM((J, I, K, L), f32), pltpu.VMEM((I, K, L), f32), pltpu.VMEM((I, K, L), f32)),
        in_specs=[anywhere] * 3,
        out_specs=(resident,) * 3,
        scratch_shapes=[
            pltpu.VMEM((2, J + 2, I + 2, K, L), f32),
            pltpu.VMEM((J, I, K, L), f32),
            pltpu.VMEM((slots, I, K, L), f32),
            pltpu.VMEM((STEPS, 2, J, I, L), f32),
            pltpu.VMEM((STEPS, 2, J, I, L), f32),
            dma((5,)),
            dma((STEPS, 2, 2)),
            dma((STEPS, 2, 2)),
            dma((STEPS, 2, 3)),
            dma((STEPS, 2, 3)),
            dma((STEPS, 2, 3)),
            dma((STEPS, 2, 3)),
            dma((slots,)),
            dma((slots,)),
            pltpu.SemaphoreType.REGULAR((2,)),
            pltpu.SemaphoreType.REGULAR((3,)),
        ],
        compiler_params=pltpu.CompilerParams(
            collective_id=0, has_side_effects=True, vmem_limit_bytes=56 * 1024 * 1024
        ),
        name="march",
    )(field_now, earlier, speed_square)
    scale = 1.0 / (J * ny)
    small = pltpu.CompilerParams(vmem_limit_bytes=16 * 1024 * 1024)

    chunks = OUT_CHUNKS if I % OUT_CHUNKS == 0 and split % OUT_CHUNKS == 0 else 1

    sums, field_end, done = pl.pallas_call(
        functools.partial(first_out_kernel, scale, chunks, split),
        out_shape=(shape, shape, pltpu.VMEM((8, L), f32)),
        in_specs=[resident] * 2,
        out_specs=(anywhere, anywhere, resident),
        scratch_shapes=[pltpu.VMEM((J, I, K, L), f32), dma((chunks,)), dma],
        compiler_params=small,
        name="first_out",
    )(end, under)
    rest = I - split
    under_rest = pl.pallas_call(
        functools.partial(rest_kernel, ny, split),
        out_shape=pltpu.VMEM((rest, K, L), f32),
        in_specs=[resident] * 3,
        out_specs=resident,
        scratch_shapes=[pltpu.VMEM((slots, rest, K, L), f32), dma((slots,)), dma((slots,))],
        compiler_params=pltpu.CompilerParams(
            collective_id=1, has_side_effects=True, vmem_limit_bytes=16 * 1024 * 1024
        ),
        name="rest",
    )(total, under, done)
    sums = pl.pallas_call(
        functools.partial(rest_out_kernel, scale, chunks, split),
        out_shape=shape,
        in_specs=[resident] * 2 + [anywhere],
        out_specs=anywhere,
        input_output_aliases={2: 0},
        scratch_shapes=[pltpu.VMEM((J, rest, K, L), f32), dma((chunks,))],
        compiler_params=small,
        name="rest_out",
    )(end, under_rest, sums)
    return sums, field_end


def solution(mesh):
    placed = P("py", "px", "pz", None)
    peers = tuple(mesh.shape[a] for a in ("py", "px", "pz"))
    return jax.shard_map(
        functools.partial(local, peers),
        mesh=mesh,
        in_specs=(placed,) * 3,
        out_specs=(placed,) * 2,
        check_vma=False,
    )
```

```python
import functools

import jax
import jax.numpy as jnp
from jax import lax
from jax.experimental import pallas as pl
from jax.experimental.pallas import tpu as pltpu
from jax.sharding import PartitionSpec as P

STEPS = 4
OUT_CHUNKS = 4
FIRST = (7, 16)
MESH = pl.DeviceIdType.MESH


def march_kernel(
    peers, split, field, before, speed, end, under, total,
    u, cs, below, ysend, yrecv,
    load_sem, x_send, x_recv, z_send, z_recv, y_send, y_recv, t_send, t_recv, word, ready,
):
    J, I, K, L = field.shape
    ny, nx, nz = peers
    my, mx, mz = (lax.axis_index(a) for a in ("py", "px", "pz"))
    y_side = ({"py": lax.rem(my + 1, ny)}, {"py": lax.rem(my + ny - 1, ny)})
    x_side = ({"px": lax.rem(mx + 1, nx)}, {"px": lax.rem(mx + nx - 1, nx)})
    z_side = ({"pz": lax.rem(mz + 1, nz)}, {"pz": lax.rem(mz + nz - 1, nz)})
    parts = ((1, J - 2), (0, 1), (J - 1, 1))
    near = I - max(I // 16, 1)
    cut = ((0, split), (split, near - split), (near, I - near))
    sent = ((0, split), (0, near), (near, I - near))
    second_core = lax.rem(mz, 2) == 1

    loads = [
        pltpu.make_async_copy(
            field.at[pl.ds(start, size)], u.at[0, pl.ds(start + 1, size), pl.ds(1, I)], load_sem.at[part]
        )
        for part, (start, size) in reversed(tuple(enumerate(parts)))
    ] + [
        pltpu.make_async_copy(before, u.at[1, pl.ds(1, J), pl.ds(1, I)], load_sem.at[3]),
        pltpu.make_async_copy(speed, cs, load_sem.at[4]),
    ]
    barrier = pltpu.get_barrier_semaphore()
    above, under_me = mx < nx - 1, mx > 0
    pairs = [(mx < nx - 1, x_side[0], mx > 0, x_side[1])]
    if nz > 1:
        pairs.append((mz < nz - 1, z_side[0], mz > 0, z_side[1]))
    if nz > 2:
        pairs.append((mz == 0, z_side[1], mz == nz - 1, z_side[0]))

    def greet(to):
        pl.semaphore_signal(barrier, inc=1, device_id=to, device_id_type=MESH)

    for d in range(1, ny):
        greet({"py": lax.rem(my + d, ny)})
    expected = ny - 1
    for has_upper, upper, has_lower, _ in pairs:
        @pl.when(has_upper)
        def _(upper=upper):
            greet(upper)

        expected = expected + jnp.where(has_lower, 1, 0)

    for load in loads[:2]:
        load.start()
    pl.semaphore_wait(barrier, expected)

    def meet():
        for n, (_, _, has_lower, lower) in enumerate(pairs):
            @pl.when(has_lower)
            def _(n=n, lower=lower):
                pl.semaphore_signal(ready.at[n], inc=1, device_id=lower, device_id_type=MESH)

        for n, (has_upper, _, _, _) in enumerate(pairs):
            @pl.when(has_upper)
            def _(n=n):
                pl.semaphore_wait(ready.at[n], 1)

    def hand_on():
        for way, (comes, goes) in enumerate(((under_me, above), (above, under_me))):
            @pl.when(comes)
            def _(way=way):
                pl.semaphore_wait(word.at[way], 1)

            @pl.when(goes)
            def _(way=way):
                pl.semaphore_signal(word.at[way], inc=1, device_id=x_side[way], device_id_type=MESH)

    def remote(src, dst, send, recv, to):
        return pltpu.make_async_remote_copy(
            src_ref=src, dst_ref=dst, send_sem=send, recv_sem=recv, device_id=to, device_id_type=MESH
        )

    def order(t):
        return (0, 1) if t % 2 == 0 else (1, 0)

    def cuts(t, side):
        return cut if t + 1 == STEPS and side == order(t)[1] else ((0, I),)

    def j_copy(t, side, c):
        row, rim = ((J - 1, 0), (0, J + 1))[side]
        start, size = cuts(t, side)[c]
        there = pl.ds(1 + start, size)
        return remote(u.at[t % 2, row + 1, there], u.at[t % 2, rim, there], x_send.at[t, side, c], x_recv.at[t, side, c], y_side[side])

    def i_copy(t, side, part):
        plane, rim = ((I - 1, 0), (0, I + 1))[side]
        start, size = parts[part]
        rows = pl.ds(start + 1, size)
        src = field.at[pl.ds(start, size), plane] if t == 0 else u.at[t % 2, rows, plane + 1]
        return remote(src, u.at[t % 2, rows, rim], z_send.at[t, side, part], z_recv.at[t, side, part], x_side[side])

    def k_copy(t, side, part):
        start, size = parts[part]
        rows = pl.ds(start, size)
        return remote(
            ysend.at[t, side, rows], yrecv.at[t, side, rows],
            y_send.at[t, side, part], y_recv.at[t, side, part], z_side[side],
        )

    def pack(t, j, i, value):
        ysend[t, 0, j, pl.ds(i, 1), :] = value[K - 1:K]
        ysend[t, 1, j, pl.ds(i, 1), :] = value[0:1]

    loads[0].wait()
    j_copy(0, 0, 0).start()
    loads[1].wait()
    j_copy(0, 1, 0).start()
    for load in loads[2:]:
        load.start()
    meet()
    hand_on()
    for part in range(3):
        for side in (0, 1):
            i_copy(0, side, part).start()

    loads[2].wait()

    def pack_row(j, carry):
        for i in range(I):
            ysend[0, 0, j, i:i + 1, :] = u[0, j + 1, i + 1, K - 1:K, :]
            ysend[0, 1, j, i:i + 1, :] = u[0, j + 1, i + 1, 0:1, :]
        return carry

    lax.fori_loop(0, J, pack_row, 0)
    for part in range(3):
        for side in (0, 1):
            k_copy(0, side, part).start()
    loads[3].wait()
    loads[4].wait()

    k_index = lax.broadcasted_iota(jnp.int32, (K, L), 0)

    def column(t, j, i):
        now, other = t % 2, (t + 1) % 2
        middle = u[now, j + 1, i + 1]
        low = jnp.where(k_index == 0, yrecv[t, 0, j, pl.ds(i, 1), :], pltpu.roll(middle, 1, 0))
        high = jnp.where(k_index == K - 1, yrecv[t, 1, j, pl.ds(i, 1), :], pltpu.roll(middle, K - 1, 0))
        spread = (
            u[now, j, i + 1] + u[now, j + 2, i + 1] + u[now, j + 1, i] + u[now, j + 1, i + 2]
            + low + high - 6.0 * middle
        )
        later = 2.0 * middle - u[other, j + 1, i + 1] + cs[j, i] * spread
        if t + 1 < STEPS:
            u[other, j + 1, i + 1] = later
            pack(t + 1, j, i, later)
        else:
            end[j, i] = later

    def total_copy(d, c):
        here = pl.ds(*sent[c])
        return remote(
            total.at[here], under.at[here] if d == 1 else below.at[d - 2, here], t_send.at[d - 1, c], t_recv.at[d - 1, c],
            {"py": lax.rem(my + d, ny)},
        )

    def for_totals(mine, c, act):
        for d in range(1, ny):
            @pl.when(jnp.logical_and(second_core if c == 0 else jnp.logical_not(second_core), my + d < ny if mine else my >= d))
            def _(d=d):
                act(total_copy(d, c), d)

    for t in range(STEPS):
        last = t + 1 == STEPS
        for side in (0, 1):
            i_copy(t, side, 0).wait_recv()
            k_copy(t, side, 0).wait_recv()
            if t > 0:
                i_copy(t - 1, side, 0).wait_send()

        def inner(q, carry, t=t):
            j = 1 + q // (I // 2)
            i = lax.rem(q, I // 2) * 2
            column(t, j, i)
            column(t, j, i + 1)
            return carry

        lax.fori_loop(0, (J - 2) * (I // 2), inner, 0)
        if not last:
            for side in (0, 1):
                i_copy(t + 1, side, 0).start()
                k_copy(t + 1, side, 0).start()

        for s in order(t):
            row, part = ((0, 1), (J - 1, 2))[s]
            for side in (0, 1):
                i_copy(t, side, part).wait_recv()
                k_copy(t, side, part).wait_recv()
                if t > 0:
                    i_copy(t - 1, side, part).wait_send()
            if t > 0:
                j_copy(t - 1, 1 - s, 0).wait_send()

            def outer(i, carry, t=t, row=row, s=s):
                column(t, row, i)
                if t + 1 == STEPS and s == order(t)[1]:
                    total[i] = total[i] + end[row, i]
                return carry

            if last and s == order(t)[1]:
                def add_up(i, carry, row=row):
                    value, *others = (end[j, i] for j in range(J) if j != row)
                    for other in others:
                        value = value + other
                    total[i] = value
                    return carry

                lax.fori_loop(0, I, add_up, 0)

            if not last:
                j_copy(t, s, 0).wait_recv()
                for c, (start, size) in enumerate(cuts(t + 1, 1 - s)):
                    lax.fori_loop(start, start + size, outer, 0)
                    j_copy(t + 1, 1 - s, c).start()
                for side in (0, 1):
                    i_copy(t + 1, side, part).start()
                    k_copy(t + 1, side, part).start()
            else:
                for c, (start, size) in enumerate(cuts(t, s)):
                    j_copy(t, s, c).wait_recv()
                    lax.fori_loop(start, start + size, outer, 0)
                    if s == order(t)[1]:
                        for_totals(True, c, lambda copy, d: copy.start())

    @pl.when(my == 0)
    def _():
        under[...] = jnp.zeros((I, K, L), jnp.float32)

    for c, (start, size) in enumerate(sent):
        def take(copy, d, here=pl.ds(start, size)):
            copy.wait_recv()
            if d > 1:
                under[here] = under[here] + below[d - 2, here]

        for_totals(False, c, take)

    for side in (0, 1):
        for c in range(len(cuts(STEPS - 1, side))):
            j_copy(STEPS - 1, side, c).wait_send()
        for part in range(3):
            i_copy(STEPS - 1, side, part).wait_send()
            for t in range(STEPS):
                k_copy(t, side, part).wait_send()
    for c in range(len(sent)):
        for_totals(True, c, lambda copy, d: copy.wait_send())


def rest_kernel(ny, split, total, _, under_rest, below, send, recv):
    size = total.shape[0] - split
    my = lax.axis_index("py")
    there = pl.ds(split, size)
    second_core = lax.rem(lax.axis_index("pz"), 2) == 1

    def copy(d):
        return pltpu.make_async_remote_copy(
            src_ref=total.at[there], dst_ref=under_rest if d == 1 else below.at[d - 2],
            send_sem=send.at[d - 1], recv_sem=recv.at[d - 1],
            device_id={"py": lax.rem(my + d, ny)}, device_id_type=MESH,
        )

    @pl.when(my == 0)
    def _():
        under_rest[...] = jnp.zeros(under_rest.shape, jnp.float32)

    @pl.when(second_core)
    def _():
        barrier = pltpu.get_barrier_semaphore()
        for d in range(1, ny):
            @pl.when(my >= d)
            def _(d=d):
                pl.semaphore_signal(barrier, inc=1, device_id={"py": lax.rem(my + ny - d, ny)}, device_id_type=MESH)

        @pl.when(my < ny - 1)
        def _():
            pl.semaphore_wait(barrier, ny - 1 - my)

        for d in range(1, ny):
            @pl.when(my + d < ny)
            def _(d=d):
                copy(d).start()

        for d in range(1, ny):
            @pl.when(my >= d)
            def _(d=d):
                copy(d).wait_recv()
                if d > 1:
                    under_rest[...] = under_rest[...] + below[d - 2]

        for d in range(1, ny):
            @pl.when(my + d < ny)
            def _(d=d):
                copy(d).wait_send()


def columns_out(scale, start, size, end, under, sums_out, csum, sem):
    J = end.shape[0]
    pieces = min(OUT_CHUNKS, size) - 1
    bounds = [0] + [1 + (size - 1) * n // max(pieces, 1) for n in range(pieces + 1)]

    def sum_copy(c):
        low, width = bounds[c], bounds[c + 1] - bounds[c]
        return pltpu.make_async_copy(
            csum.at[:, pl.ds(low, width)], sums_out.at[:, pl.ds(start + low, width)], sem.at[c]
        )

    for c in range(pieces + 1):
        def running(i, carry):
            value = under[i]
            for j in range(J):
                value = value + end[j, start + i]
                csum[j, i] = value * scale
            return carry

        lax.fori_loop(bounds[c], bounds[c + 1], running, 0)
        sum_copy(c).start()
    return [sum_copy(c) for c in range(pieces + 1)]


def first_out_kernel(scale, split, end, under, sums_out, field_out, done, csum, sem, field_sem):
    whole = pltpu.make_async_copy(end, field_out, field_sem)
    whole.start()
    partly = jnp.logical_and(lax.rem(lax.axis_index("pz"), 2) == 1, lax.axis_index("py") > 0)

    def columns(size):
        for copy in columns_out(scale, 0, size, end, under, sums_out, csum, sem):
            copy.wait()

    @pl.when(partly)
    def _():
        columns(split)

    @pl.when(jnp.logical_not(partly))
    def _():
        columns(end.shape[1])

    whole.wait()
    done[...] = jnp.zeros(done.shape, jnp.float32)


def rest_out_kernel(scale, split, end, under_rest, _, sums_out, csum, sem):
    @pl.when(jnp.logical_and(lax.rem(lax.axis_index("pz"), 2) == 1, lax.axis_index("py") > 0))
    def _():
        for copy in columns_out(scale, split, end.shape[1] - split, end, under_rest, sums_out, csum, sem):
            copy.wait()


def local(peers, field_now, earlier, speed_square):
    J, I, K, L = field_now.shape
    ny = peers[0]
    split = I * FIRST[0] // FIRST[1]
    f32 = jnp.float32
    dma = pltpu.SemaphoreType.DMA
    anywhere = pl.BlockSpec(memory_space=pltpu.MemorySpace.HBM)
    shape = jax.ShapeDtypeStruct(field_now.shape, f32)
    slots, extra = max(ny - 1, 1), max(ny - 2, 1)
    resident = pl.BlockSpec(memory_space=pltpu.VMEM)
    end, under, total = pl.pallas_call(
        functools.partial(march_kernel, peers, split),
        out_shape=(pltpu.VMEM((J, I, K, L), f32), pltpu.VMEM((I, K, L), f32), pltpu.VMEM((I, K, L), f32)),
        in_specs=[anywhere] * 3,
        out_specs=(resident,) * 3,
        scratch_shapes=[
            pltpu.VMEM((2, J + 2, I + 2, K, L), f32),
            pltpu.VMEM((J, I, K, L), f32),
            pltpu.VMEM((extra, I, K, L), f32),
            pltpu.VMEM((STEPS, 2, J, I, L), f32),
            pltpu.VMEM((STEPS, 2, J, I, L), f32),
            dma((5,)),
            dma((STEPS, 2, 3)),
            dma((STEPS, 2, 3)),
            dma((STEPS, 2, 3)),
            dma((STEPS, 2, 3)),
            dma((STEPS, 2, 3)),
            dma((STEPS, 2, 3)),
            dma((slots, 3)),
            dma((slots, 3)),
            pltpu.SemaphoreType.REGULAR((2,)),
            pltpu.SemaphoreType.REGULAR((3,)),
        ],
        compiler_params=pltpu.CompilerParams(
            collective_id=0, has_side_effects=True, vmem_limit_bytes=56 * 1024 * 1024
        ),
        name="march",
    )(field_now, earlier, speed_square)
    scale = 1.0 / (J * ny)
    small = pltpu.CompilerParams(vmem_limit_bytes=16 * 1024 * 1024)

    sums, field_end, done = pl.pallas_call(
        functools.partial(first_out_kernel, scale, split),
        out_shape=(shape, shape, pltpu.VMEM((8, L), f32)),
        in_specs=[resident] * 2,
        out_specs=(anywhere, anywhere, resident),
        scratch_shapes=[pltpu.VMEM((J, I, K, L), f32), dma((OUT_CHUNKS,)), dma],
        compiler_params=small,
        name="first_out",
    )(end, under)
    rest = I - split
    under_rest = pl.pallas_call(
        functools.partial(rest_kernel, ny, split),
        out_shape=pltpu.VMEM((rest, K, L), f32),
        in_specs=[resident] * 2,
        out_specs=resident,
        scratch_shapes=[pltpu.VMEM((extra, rest, K, L), f32), dma((slots,)), dma((slots,))],
        compiler_params=pltpu.CompilerParams(
            collective_id=1, has_side_effects=True, vmem_limit_bytes=16 * 1024 * 1024
        ),
        name="rest",
    )(total, done)
    sums = pl.pallas_call(
        functools.partial(rest_out_kernel, scale, split),
        out_shape=shape,
        in_specs=[resident] * 2 + [anywhere],
        out_specs=anywhere,
        input_output_aliases={2: 0},
        scratch_shapes=[pltpu.VMEM((J, rest, K, L), f32), dma((OUT_CHUNKS,))],
        compiler_params=small,
        name="rest_out",
    )(end, under_rest, sums)
    return sums, field_end


def solution(mesh):
    placed = P("py", "px", "pz", None)
    peers = tuple(mesh.shape[a] for a in ("py", "px", "pz"))
    return jax.shard_map(
        functools.partial(local, peers),
        mesh=mesh,
        in_specs=(placed,) * 3,
        out_specs=(placed,) * 2,
        check_vma=False,
    )
```

```python
import functools

import jax
import jax.numpy as jnp
from jax import lax
from jax.experimental import pallas as pl
from jax.experimental.pallas import tpu as pltpu
from jax.sharding import PartitionSpec as P

STEPS = 4
OUT_CHUNKS = 4
FIRST = (3, 8)
MESH = pl.DeviceIdType.MESH


def march_kernel(
    peers, split, field, before, speed, end, under, total,
    u, cs, below, ysend, yrecv,
    load_sem, x_send, x_recv, z_send, z_recv, y_send, y_recv, t_send, t_recv, word, ready,
):
    J, I, K, L = field.shape
    ny, nx, nz = peers
    my, mx, mz = (lax.axis_index(a) for a in ("py", "px", "pz"))
    y_side = ({"py": lax.rem(my + 1, ny)}, {"py": lax.rem(my + ny - 1, ny)})
    x_side = ({"px": lax.rem(mx + 1, nx)}, {"px": lax.rem(mx + nx - 1, nx)})
    z_side = ({"pz": lax.rem(mz + 1, nz)}, {"pz": lax.rem(mz + nz - 1, nz)})
    parts = ((1, J - 2), (0, 1), (J - 1, 1))
    near = I - max(I // 16, 1)
    cut = ((0, split), (split, near - split), (near, I - near))
    sent = ((0, split), (0, near), (near, I - near))
    second_core = lax.rem(mz, 2) == 1

    loads = [
        pltpu.make_async_copy(
            field.at[pl.ds(start, size)], u.at[0, pl.ds(start + 1, size), pl.ds(1, I)], load_sem.at[part]
        )
        for part, (start, size) in reversed(tuple(enumerate(parts)))
    ] + [
        pltpu.make_async_copy(before, u.at[1, pl.ds(1, J), pl.ds(1, I)], load_sem.at[3]),
        pltpu.make_async_copy(speed, cs, load_sem.at[4]),
    ]
    barrier = pltpu.get_barrier_semaphore()
    above, under_me = mx < nx - 1, mx > 0
    pairs = [(mx < nx - 1, x_side[0], mx > 0, x_side[1])]
    if nz > 1:
        pairs.append((mz < nz - 1, z_side[0], mz > 0, z_side[1]))
    if nz > 2:
        pairs.append((mz == 0, z_side[1], mz == nz - 1, z_side[0]))

    def greet(to):
        pl.semaphore_signal(barrier, inc=1, device_id=to, device_id_type=MESH)

    for d in range(1, ny):
        greet({"py": lax.rem(my + d, ny)})
    expected = ny - 1
    for has_upper, upper, has_lower, _ in pairs:
        @pl.when(has_upper)
        def _(upper=upper):
            greet(upper)

        expected = expected + jnp.where(has_lower, 1, 0)

    for load in loads[:2]:
        load.start()
    pl.semaphore_wait(barrier, expected)

    def meet():
        for n, (_, _, has_lower, lower) in enumerate(pairs):
            @pl.when(has_lower)
            def _(n=n, lower=lower):
                pl.semaphore_signal(ready.at[n], inc=1, device_id=lower, device_id_type=MESH)

        for n, (has_upper, _, _, _) in enumerate(pairs):
            @pl.when(has_upper)
            def _(n=n):
                pl.semaphore_wait(ready.at[n], 1)

    def hand_on():
        for way, (comes, goes) in enumerate(((under_me, above), (above, under_me))):
            @pl.when(comes)
            def _(way=way):
                pl.semaphore_wait(word.at[way], 1)

            @pl.when(goes)
            def _(way=way):
                pl.semaphore_signal(word.at[way], inc=1, device_id=x_side[way], device_id_type=MESH)

    def remote(src, dst, send, recv, to):
        return pltpu.make_async_remote_copy(
            src_ref=src, dst_ref=dst, send_sem=send, recv_sem=recv, device_id=to, device_id_type=MESH
        )

    def order(t):
        return (0, 1) if t % 2 == 0 else (1, 0)

    def cuts(t, side):
        return cut if t + 1 == STEPS and side == order(t)[1] else ((0, I),)

    def j_copy(t, side, c):
        row, rim = ((J - 1, 0), (0, J + 1))[side]
        start, size = cuts(t, side)[c]
        there = pl.ds(1 + start, size)
        return remote(u.at[t % 2, row + 1, there], u.at[t % 2, rim, there], x_send.at[t, side, c], x_recv.at[t, side, c], y_side[side])

    def i_copy(t, side, part):
        plane, rim = ((I - 1, 0), (0, I + 1))[side]
        start, size = parts[part]
        rows = pl.ds(start + 1, size)
        src = field.at[pl.ds(start, size), plane] if t == 0 else u.at[t % 2, rows, plane + 1]
        return remote(src, u.at[t % 2, rows, rim], z_send.at[t, side, part], z_recv.at[t, side, part], x_side[side])

    def k_copy(t, side, part):
        start, size = parts[part]
        rows = pl.ds(start, size)
        return remote(
            ysend.at[t, side, rows], yrecv.at[t, side, rows],
            y_send.at[t, side, part], y_recv.at[t, side, part], z_side[side],
        )

    def pack(t, j, i, value):
        ysend[t, 0, j, pl.ds(i, 1), :] = value[K - 1:K]
        ysend[t, 1, j, pl.ds(i, 1), :] = value[0:1]

    loads[0].wait()
    j_copy(0, 0, 0).start()
    loads[1].wait()
    j_copy(0, 1, 0).start()
    for load in loads[2:]:
        load.start()
    meet()
    hand_on()
    for part in range(3):
        for side in (0, 1):
            i_copy(0, side, part).start()

    loads[2].wait()

    def pack_row(j, carry):
        for i in range(I):
            ysend[0, 0, j, i:i + 1, :] = u[0, j + 1, i + 1, K - 1:K, :]
            ysend[0, 1, j, i:i + 1, :] = u[0, j + 1, i + 1, 0:1, :]
        return carry

    lax.fori_loop(0, J, pack_row, 0)
    for part in range(3):
        for side in (0, 1):
            k_copy(0, side, part).start()
    loads[3].wait()
    loads[4].wait()

    k_index = lax.broadcasted_iota(jnp.int32, (K, L), 0)

    def column(t, j, i):
        now, other = t % 2, (t + 1) % 2
        middle = u[now, j + 1, i + 1]
        low = jnp.where(k_index == 0, yrecv[t, 0, j, pl.ds(i, 1), :], pltpu.roll(middle, 1, 0))
        high = jnp.where(k_index == K - 1, yrecv[t, 1, j, pl.ds(i, 1), :], pltpu.roll(middle, K - 1, 0))
        spread = (
            u[now, j, i + 1] + u[now, j + 2, i + 1] + u[now, j + 1, i] + u[now, j + 1, i + 2]
            + low + high - 6.0 * middle
        )
        later = 2.0 * middle - u[other, j + 1, i + 1] + cs[j, i] * spread
        if t + 1 < STEPS:
            u[other, j + 1, i + 1] = later
            pack(t + 1, j, i, later)
        else:
            end[j, i] = later

    def total_copy(d, c):
        here = pl.ds(*sent[c])
        return remote(
            total.at[here], under.at[here] if d == 1 else below.at[d - 2, here], t_send.at[d - 1, c], t_recv.at[d - 1, c],
            {"py": lax.rem(my + d, ny)},
        )

    def for_totals(mine, c, act):
        for d in range(1, ny):
            @pl.when(jnp.logical_and(second_core if c == 0 else jnp.logical_not(second_core), my + d < ny if mine else my >= d))
            def _(d=d):
                act(total_copy(d, c), d)

    for t in range(STEPS):
        last = t + 1 == STEPS
        for side in (0, 1):
            i_copy(t, side, 0).wait_recv()
            k_copy(t, side, 0).wait_recv()
            if t > 0:
                i_copy(t - 1, side, 0).wait_send()

        def inner(q, carry, t=t):
            j = 1 + q // (I // 2)
            i = lax.rem(q, I // 2) * 2
            column(t, j, i)
            column(t, j, i + 1)
            return carry

        lax.fori_loop(0, (J - 2) * (I // 2), inner, 0)
        if not last:
            for side in (0, 1):
                i_copy(t + 1, side, 0).start()
                k_copy(t + 1, side, 0).start()

        for s in order(t):
            row, part = ((0, 1), (J - 1, 2))[s]
            for side in (0, 1):
                i_copy(t, side, part).wait_recv()
                k_copy(t, side, part).wait_recv()
                if t > 0:
                    i_copy(t - 1, side, part).wait_send()
            if t > 0:
                j_copy(t - 1, 1 - s, 0).wait_send()

            def outer(i, carry, t=t, row=row, s=s):
                column(t, row, i)
                if t + 1 == STEPS and s == order(t)[1]:
                    total[i] = total[i] + end[row, i]
                return carry

            if last and s == order(t)[1]:
                def add_up(i, carry, row=row):
                    value, *others = (end[j, i] for j in range(J) if j != row)
                    for other in others:
                        value = value + other
                    total[i] = value
                    return carry

                lax.fori_loop(0, I, add_up, 0)

            if not last:
                j_copy(t, s, 0).wait_recv()
                for c, (start, size) in enumerate(cuts(t + 1, 1 - s)):
                    lax.fori_loop(start, start + size, outer, 0)
                    j_copy(t + 1, 1 - s, c).start()
                for side in (0, 1):
                    i_copy(t + 1, side, part).start()
                    k_copy(t + 1, side, part).start()
            else:
                for c, (start, size) in enumerate(cuts(t, s)):
                    j_copy(t, s, c).wait_recv()
                    lax.fori_loop(start, start + size, outer, 0)
                    if s == order(t)[1]:
                        for_totals(True, c, lambda copy, d: copy.start())

    @pl.when(my == 0)
    def _():
        under[...] = jnp.zeros((I, K, L), jnp.float32)

    for c, (start, size) in enumerate(sent):
        def take(copy, d, here=pl.ds(start, size)):
            copy.wait_recv()
            if d > 1:
                under[here] = under[here] + below[d - 2, here]

        for_totals(False, c, take)

    for side in (0, 1):
        for c in range(len(cuts(STEPS - 1, side))):
            j_copy(STEPS - 1, side, c).wait_send()
        for part in range(3):
            i_copy(STEPS - 1, side, part).wait_send()
            for t in range(STEPS):
                k_copy(t, side, part).wait_send()
    for c in range(len(sent)):
        for_totals(True, c, lambda copy, d: copy.wait_send())


def rest_kernel(ny, split, total, _, under_rest, below, send, recv):
    size = total.shape[0] - split
    my = lax.axis_index("py")
    there = pl.ds(split, size)
    second_core = lax.rem(lax.axis_index("pz"), 2) == 1

    def copy(d):
        return pltpu.make_async_remote_copy(
            src_ref=total.at[there], dst_ref=under_rest if d == 1 else below.at[d - 2],
            send_sem=send.at[d - 1], recv_sem=recv.at[d - 1],
            device_id={"py": lax.rem(my + d, ny)}, device_id_type=MESH,
        )

    @pl.when(my == 0)
    def _():
        under_rest[...] = jnp.zeros(under_rest.shape, jnp.float32)

    @pl.when(second_core)
    def _():
        barrier = pltpu.get_barrier_semaphore()
        for d in range(1, ny):
            @pl.when(my >= d)
            def _(d=d):
                pl.semaphore_signal(barrier, inc=1, device_id={"py": lax.rem(my + ny - d, ny)}, device_id_type=MESH)

        @pl.when(my < ny - 1)
        def _():
            pl.semaphore_wait(barrier, ny - 1 - my)

        for d in range(1, ny):
            @pl.when(my + d < ny)
            def _(d=d):
                copy(d).start()

        for d in range(1, ny):
            @pl.when(my >= d)
            def _(d=d):
                copy(d).wait_recv()
                if d > 1:
                    under_rest[...] = under_rest[...] + below[d - 2]

        for d in range(1, ny):
            @pl.when(my + d < ny)
            def _(d=d):
                copy(d).wait_send()


def columns_out(scale, start, size, end, under, sums_out, csum, sem):
    J = end.shape[0]
    pieces = min(OUT_CHUNKS, size) - 1
    bounds = [0] + [1 + (size - 1) * n // max(pieces, 1) for n in range(pieces + 1)]

    def sum_copy(c):
        low, width = bounds[c], bounds[c + 1] - bounds[c]
        return pltpu.make_async_copy(
            csum.at[:, pl.ds(low, width)], sums_out.at[:, pl.ds(start + low, width)], sem.at[c]
        )

    for c in range(pieces + 1):
        def running(i, carry):
            value = under[i]
            for j in range(J):
                value = value + end[j, start + i]
                csum[j, i] = value * scale
            return carry

        lax.fori_loop(bounds[c], bounds[c + 1], running, 0)
        sum_copy(c).start()
    return [sum_copy(c) for c in range(pieces + 1)]


def first_out_kernel(scale, split, end, under, sums_out, field_out, done, csum, sem, field_sem):
    whole = pltpu.make_async_copy(end, field_out, field_sem)
    whole.start()
    partly = jnp.logical_and(lax.rem(lax.axis_index("pz"), 2) == 1, lax.axis_index("py") > 0)

    def columns(size):
        for copy in columns_out(scale, 0, size, end, under, sums_out, csum, sem):
            copy.wait()

    @pl.when(partly)
    def _():
        columns(split)

    @pl.when(jnp.logical_not(partly))
    def _():
        columns(end.shape[1])

    whole.wait()
    done[...] = jnp.zeros(done.shape, jnp.float32)


def rest_out_kernel(scale, split, end, under_rest, _, sums_out, csum, sem):
    @pl.when(jnp.logical_and(lax.rem(lax.axis_index("pz"), 2) == 1, lax.axis_index("py") > 0))
    def _():
        for copy in columns_out(scale, split, end.shape[1] - split, end, under_rest, sums_out, csum, sem):
            copy.wait()


def local(peers, field_now, earlier, speed_square):
    J, I, K, L = field_now.shape
    ny = peers[0]
    split = I * FIRST[0] // FIRST[1]
    f32 = jnp.float32
    dma = pltpu.SemaphoreType.DMA
    anywhere = pl.BlockSpec(memory_space=pltpu.MemorySpace.HBM)
    shape = jax.ShapeDtypeStruct(field_now.shape, f32)
    slots, extra = max(ny - 1, 1), max(ny - 2, 1)
    resident = pl.BlockSpec(memory_space=pltpu.VMEM)
    end, under, total = pl.pallas_call(
        functools.partial(march_kernel, peers, split),
        out_shape=(pltpu.VMEM((J, I, K, L), f32), pltpu.VMEM((I, K, L), f32), pltpu.VMEM((I, K, L), f32)),
        in_specs=[anywhere] * 3,
        out_specs=(resident,) * 3,
        scratch_shapes=[
            pltpu.VMEM((2, J + 2, I + 2, K, L), f32),
            pltpu.VMEM((J, I, K, L), f32),
            pltpu.VMEM((extra, I, K, L), f32),
            pltpu.VMEM((STEPS, 2, J, I, L), f32),
            pltpu.VMEM((STEPS, 2, J, I, L), f32),
            dma((5,)),
            dma((STEPS, 2, 3)),
            dma((STEPS, 2, 3)),
            dma((STEPS, 2, 3)),
            dma((STEPS, 2, 3)),
            dma((STEPS, 2, 3)),
            dma((STEPS, 2, 3)),
            dma((slots, 3)),
            dma((slots, 3)),
            pltpu.SemaphoreType.REGULAR((2,)),
            pltpu.SemaphoreType.REGULAR((3,)),
        ],
        compiler_params=pltpu.CompilerParams(
            collective_id=0, has_side_effects=True, vmem_limit_bytes=56 * 1024 * 1024
        ),
        name="march",
    )(field_now, earlier, speed_square)
    scale = 1.0 / (J * ny)
    small = pltpu.CompilerParams(vmem_limit_bytes=16 * 1024 * 1024)

    sums, field_end, done = pl.pallas_call(
        functools.partial(first_out_kernel, scale, split),
        out_shape=(shape, shape, pltpu.VMEM((8, L), f32)),
        in_specs=[resident] * 2,
        out_specs=(anywhere, anywhere, resident),
        scratch_shapes=[pltpu.VMEM((J, I, K, L), f32), dma((OUT_CHUNKS,)), dma],
        compiler_params=small,
        name="first_out",
    )(end, under)
    rest = I - split
    under_rest = pl.pallas_call(
        functools.partial(rest_kernel, ny, split),
        out_shape=pltpu.VMEM((rest, K, L), f32),
        in_specs=[resident] * 2,
        out_specs=resident,
        scratch_shapes=[pltpu.VMEM((extra, rest, K, L), f32), dma((slots,)), dma((slots,))],
        compiler_params=pltpu.CompilerParams(
            collective_id=1, has_side_effects=True, vmem_limit_bytes=16 * 1024 * 1024
        ),
        name="rest",
    )(total, done)
    sums = pl.pallas_call(
        functools.partial(rest_out_kernel, scale, split),
        out_shape=shape,
        in_specs=[resident] * 2 + [anywhere],
        out_specs=anywhere,
        input_output_aliases={2: 0},
        scratch_shapes=[pltpu.VMEM((J, rest, K, L), f32), dma((OUT_CHUNKS,))],
        compiler_params=small,
        name="rest_out",
    )(end, under_rest, sums)
    return sums, field_end


def solution(mesh):
    placed = P("py", "px", "pz", None)
    peers = tuple(mesh.shape[a] for a in ("py", "px", "pz"))
    return jax.shard_map(
        functools.partial(local, peers),
        mesh=mesh,
        in_specs=(placed,) * 3,
        out_specs=(placed,) * 2,
        check_vma=False,
    )
```
